128 devices in a mesh: row: 8 (over z, core), col: 16 (over x, y).
Axes of the slice: x: 4, y: 4, z: 4, core: 2. Of those that a mesh axis runs over, the one named last changes fastest.
Arguments:
- tiles: bfloat16 [8, 16, 128, 128, 128], P('row', 'col'), may hold values from -6 to 6
- tile_row: int32 [8, 16, 128], P('row', 'col'), may hold values from 0 to 127, as said below
- tile_col: int32 [8, 16, 128], P('row', 'col'), may hold values from 0 to 63
- tile_count: int32 [8, 16], P('row', 'col'), may hold values from 16 to 128, as said below
- query_ids: int32 [128], replicated, may hold values from 0 to 131071
- damping: float32 [128], replicated, may hold values from 0.006629126 to 0.026516505
Outputs:
- scores: float32 [131072, 128], P(('row', 'col'))
The draws below stay inside these ranges and needn't reach their ends.
Inputs may be any that keep to these rules, and one draw needn't show every extreme that they name: `tile_count`: some device holds exactly 128 live slots; slots at or past the count hold arbitrary finite values and are ignored. `tile_row`: positions may repeat within a device; such tiles add. For every device and every col index o, the live slots name at most 4 distinct values among o * 8 to o * 8 + 7, and every device reaches 4 for some o. `query_ids`: ids may repeat.
All inputs are finite; a program needn't handle non-finite values.
Results may differ from the reference program's by a relative error of at most 0.003.
Values may be sent and summed in bfloat16 or wider, within the bound.
No kernel may reach another device: no remote copies, remote signals or barrier semaphores. Data moves between devices by JAX's collectives and lax.ppermute only.
A program may use at most 128 MiB of HBM per device.

```python
import math
import jax
import jax.numpy as jnp
from jax import lax

TILE = 128
BPD = 8
TILES_DEV = 128
QUERIES = 128
TERMS = 4
TOUCH = 4
NBLK = 1024
NODES = 131072
N_ROW = 8
N_COL = 16


def draw_tile_count(key, part):
    shifts = jax.random.randint(key, (N_ROW * N_COL,), 0, 4)
    counts = jnp.right_shift(jnp.full((N_ROW * N_COL,), TILES_DEV, jnp.int32), shifts.astype(jnp.int32))
    fullest = jax.random.randint(jax.random.fold_in(key, 7), (), 0, N_ROW * N_COL)
    counts = counts.at[fullest].set(TILES_DEV)
    return counts.reshape(N_ROW, N_COL).astype(jnp.int32)


def draw_tile_row(key, part):
    devs = N_ROW * N_COL
    owners = jax.random.randint(jax.random.fold_in(key, 11), (devs, TILES_DEV), 0, N_COL)
    starts = jax.random.randint(jax.random.fold_in(key, 12), (devs, N_COL), 0, BPD)
    offsets = jax.random.randint(jax.random.fold_in(key, 13), (devs, TILES_DEV), 0, TOUCH)
    favoured = jax.random.randint(jax.random.fold_in(key, 14), (devs,), 0, N_COL)
    slot = jnp.arange(TILES_DEV, dtype=jnp.int32)
    first = slot < TOUCH
    owners = jnp.where(first[None, :], favoured[:, None], owners)
    offsets = jnp.where(first[None, :], slot[None, :], offsets)
    chosen = jnp.take_along_axis(starts, owners, axis=1)
    local = (chosen + offsets) % BPD
    return (owners * BPD + local).reshape(N_ROW, N_COL, TILES_DEV).astype(jnp.int32)


def with_ends(array, stream_key, low, top_value):
    longest = array.shape.index(max(array.shape))
    spots = []
    for shift in (0, 1):
        where = [jax.random.randint(jax.random.fold_in(stream_key, axis), (), 0, length) for axis, length in enumerate(array.shape)]
        where[longest] = (where[longest] + shift) % array.shape[longest]
        spots.append(tuple(where))
    return array.at[spots[0]].set(low).at[spots[1]].set(top_value)


def levels(key, extent, pieces, least, largest):
    loudness, own = 1.0, jax.random.fold_in(key, 6)
    for dim, shards_of in pieces:
        steps = jnp.exp(jax.random.uniform(jax.random.fold_in(own, dim), (shards_of,), jnp.float32, least / len(pieces), largest / len(pieces)))
        loudness = loudness * jnp.repeat(steps, extent[dim] // shards_of).reshape([-1 if axis == dim else 1 for axis in range(len(extent))])
    return loudness


def normal_values(key, extent, scale, bound, cuts=(), kind=jnp.bfloat16):
    entries = scale * jax.random.normal(key, extent, jnp.float32)
    if cuts:
        entries = entries * levels(key, extent, cuts, -0.22, 0.18)
    return jnp.clip(entries, -bound, bound).astype(kind)


def setup_inputs(seed: int = 0) -> dict:
    keys = jax.random.split(jax.random.key(seed), 7)
    return {
        "tiles": normal_values(keys[0], (N_ROW, N_COL, TILES_DEV, TILE, TILE), 1.0, 6.0, ((0, 8), (1, 16))),
        "tile_row": draw_tile_row(jax.random.fold_in(keys[6], 71), 0),
        "tile_col": with_ends(jax.random.randint(keys[2], (N_ROW, N_COL, TILES_DEV), 0, BPD * N_ROW), jax.random.fold_in(keys[2], 1), 0, (BPD * N_ROW) - 1).astype(jnp.int32),
        "tile_count": draw_tile_count(jax.random.fold_in(keys[6], 71), 0),
        "query_ids": with_ends(jax.random.randint(keys[4], (QUERIES,), 0, NODES), jax.random.fold_in(keys[4], 1), 0, NODES - 1).astype(jnp.int32),
        "damping": jnp.clip(jnp.exp(jax.random.uniform(keys[5], (QUERIES,), jnp.float32, math.log(0.006629126), math.log(0.026516505))), 0.006629126, 0.026516505),
    }


def device_partial(tile_block, rows, cols, count, xcol):
    picked = xcol[cols]
    prod = jnp.einsum("tab,tbq->taq", tile_block.astype(jnp.float32), picked.astype(jnp.float32))
    live = (jnp.arange(tile_block.shape[0], dtype=jnp.int32) < count).astype(jnp.float32)
    prod = prod * live[:, None, None]
    return jax.ops.segment_sum(prod, rows, num_segments=BPD * N_COL)


def reference(tiles, tile_row, tile_col, tile_count, query_ids, damping):
    nodes = NBLK * TILE
    queries = query_ids.shape[0]
    node_ids = jnp.arange(nodes, dtype=jnp.int32)
    xvec = (node_ids[:, None] == query_ids[None, :]).astype(jnp.bfloat16)
    scores = jnp.zeros((nodes, queries), jnp.float32)
    coef = jnp.ones((queries,), jnp.float32)
    for step in range(TERMS):
        xgrid = xvec.reshape(N_ROW, N_COL, BPD, TILE, queries)

        def one_row(ridx):
            def add_col(cidx, total):
                xcol = lax.dynamic_index_in_dim(xgrid, cidx, 1, keepdims=False)
                xcol = xcol.reshape(N_ROW * BPD, TILE, queries)
                tblock = tiles[ridx, cidx]
                part = device_partial(tblock, tile_row[ridx, cidx], tile_col[ridx, cidx], tile_count[ridx, cidx], xcol)
                rounded = lax.optimization_barrier(part.astype(jnp.bfloat16))
                return total + rounded.astype(jnp.float32)

            start = jnp.zeros((BPD * N_COL, TILE, queries), jnp.float32)
            return lax.fori_loop(0, N_COL, add_col, start)

        ysum = lax.map(one_row, jnp.arange(N_ROW, dtype=jnp.int32))
        ysum = ysum.reshape(nodes, queries)
        scores = scores + coef[None, :] * ysum
        coef = coef * damping
        xvec = ysum.astype(jnp.bfloat16)
    return scores
```

```python
import jax
import jax.numpy as jnp
from jax import lax
from jax.experimental import pallas as pl
from jax.experimental.pallas import tpu as pltpu
from jax.sharding import PartitionSpec as P

BPD = 8
TERMS = 4
TOUCH = 4
N_Z = 4
N_CORE = 2
STREAMS = 2
UNROLL = 8

VMEM = pl.BlockSpec(memory_space=pltpu.VMEM)
SMEM = pl.BlockSpec(memory_space=pltpu.SMEM)


def product_kernel(parts):
    def body(slot_ref, place_ref, count_ref, tiles_ref, *refs):
        x_refs, (out_ref, acc_ref, x_ref) = refs[:parts], refs[parts:]
        each = x_ref.shape[0] // parts
        for part in range(parts):
            x_ref[part * each : (part + 1) * each] = x_refs[part][...]
        acc_ref[...] = jnp.zeros(acc_ref.shape, jnp.float32)

        def group(index, carry):
            base = index * UNROLL
            prods = []
            for lane in range(UNROLL):
                xblock = x_ref[place_ref[base + lane]]
                prods.append(
                    lax.dot_general(
                        xblock,
                        tiles_ref[base + lane],
                        (((1,), (1,)), ((), ())),
                        preferred_element_type=jnp.float32,
                    )
                )
            for lane in range(UNROLL):
                slot = slot_ref[base + lane]
                acc_ref[slot] = acc_ref[slot] + prods[lane]
            return carry

        lax.fori_loop(0, (count_ref[0] + UNROLL - 1) // UNROLL, group, 0)
        out_ref[...] = acc_ref[: out_ref.shape[0]].astype(jnp.bfloat16)

    return body


def products(slots, places, count, tiles, xparts, sent):
    parts = len(xparts)
    each, width, tile = xparts[0].shape
    return pl.pallas_call(
        product_kernel(parts),
        out_shape=jax.ShapeDtypeStruct((sent, width, tile), jnp.bfloat16),
        in_specs=[SMEM, SMEM, SMEM, VMEM] + [VMEM] * parts,
        out_specs=VMEM,
        scratch_shapes=[
            pltpu.VMEM((sent + 1, width, tile), jnp.float32),
            pltpu.VMEM((parts * each, width, tile), jnp.bfloat16),
        ],
        name="products",
    )(slots, places, count, tiles, *xparts)


def owned_kernel(id_ref, got_ref, coef_ref, score_ref, x_ref, out_ref, acc_ref):
    acc_ref[...] = jnp.zeros(acc_ref.shape, jnp.float32)
    for index in range(got_ref.shape[0]):
        block = id_ref[index]
        acc_ref[block] = acc_ref[block] + got_ref[index].astype(jnp.float32)
    owned = acc_ref[: out_ref.shape[0]]
    x_ref[...] = owned.astype(jnp.bfloat16)
    out_ref[...] = score_ref[...] + coef_ref[...][None] * owned


def owned_sum(ids, got, coef, scores):
    blocks, width, tile = scores.shape
    return pl.pallas_call(
        owned_kernel,
        out_shape=(
            jax.ShapeDtypeStruct(scores.shape, jnp.bfloat16),
            jax.ShapeDtypeStruct(scores.shape, jnp.float32),
        ),
        in_specs=[SMEM, VMEM, VMEM, VMEM],
        out_specs=(VMEM, VMEM),
        scratch_shapes=[pltpu.VMEM((blocks + 1, width, tile), jnp.float32)],
        name="owned",
    )(ids, got, coef, scores)


def row_shift(dz, dcore):
    return [
        (z * N_CORE + core, (z + dz) % N_Z * N_CORE + (core + dcore) % N_CORE)
        for z in range(N_Z)
        for core in range(N_CORE)
    ]


def column_parts(mine):
    same = [mine] + [lax.ppermute(mine, "row", row_shift(dz, 0)) for dz in range(1, N_Z)]
    other = [lax.ppermute(part, "row", row_shift(0, 1)) for part in same]
    return same + other


def routes(rows, cols, count, n_col):
    slots = rows.shape[0]
    live = jnp.arange(slots, dtype=jnp.int32) < count
    blocks = jnp.arange(n_col * BPD, dtype=jnp.int32)
    hits = (rows[None, :] == blocks[:, None]) & live[None, :]
    marked = jnp.any(hits, axis=1).astype(jnp.int32).reshape(n_col, BPD)
    local = jnp.arange(BPD, dtype=jnp.int32)
    rank = jnp.sum(marked[:, None, :] * (local[None, None, :] < local[None, :, None]), axis=2)
    slot_of = (jnp.arange(n_col, dtype=jnp.int32)[:, None] * TOUCH + rank).reshape(-1)
    slot = jnp.sum(jnp.where(hits, slot_of[:, None], 0), axis=0)
    slot = jnp.where(live, slot, n_col * TOUCH)
    places = jnp.arange(TOUCH, dtype=jnp.int32)
    select = (marked[:, None, :] > 0) & (rank[:, None, :] == places[None, :, None])
    ids = jnp.sum(jnp.where(select, local[None, None, :] - BPD, 0), axis=2) + BPD
    row = lax.axis_index("row")
    owner, block = cols // BPD, cols % BPD
    far = (row // N_CORE - owner // N_CORE) % N_Z
    place = ((row % N_CORE != owner % N_CORE).astype(jnp.int32) * N_Z + far) * BPD + block
    return slot, place, ids


def shards(tiles, tile_row, tile_col, tile_count, query_ids, damping):
    tiles = tiles[0, 0]
    tile = tiles.shape[1]
    count = tile_count[0, 0]
    n_row, n_col = lax.axis_size("row"), lax.axis_size("col")
    slot, place, ids = routes(tile_row[0, 0], tile_col[0, 0], count, n_col)
    got_ids = lax.all_to_all(ids, "col", split_axis=0, concat_axis=0, tiled=True).reshape(-1)
    count = count.reshape(1)
    width = query_ids.shape[0] // STREAMS
    row, col = lax.axis_index("row"), lax.axis_index("col")
    part = jnp.arange(n_row * BPD, dtype=jnp.int32) // BPD
    core = (row + part // N_Z) % N_CORE
    z = (row // N_CORE - part) % N_Z
    block = ((z * N_CORE + core) * n_col + col) * BPD + jnp.arange(n_row * BPD, dtype=jnp.int32) % BPD
    nodes = block[:, None, None] * tile + jnp.arange(tile, dtype=jnp.int32)[None, None, :]
    xparts, scores = [], []
    for stream in range(STREAMS):
        asked = query_ids[stream * width : (stream + 1) * width]
        xparts.append([(nodes == asked[None, :, None]).astype(jnp.bfloat16)])
        scores.append(jnp.zeros((BPD, width, tile), jnp.float32))
    coef = jnp.ones_like(damping)
    for step in range(TERMS):
        wide = jnp.broadcast_to(coef[:, None], (coef.shape[0], tile))
        coef = coef * damping
        for stream in range(STREAMS):
            with jax.named_scope(f"t{step}s{stream}"):
                sent = products(slot, place, count, tiles, xparts[stream], n_col * TOUCH)
                got = lax.all_to_all(sent, "col", split_axis=0, concat_axis=0, tiled=True)
                mine, scores[stream] = owned_sum(
                    got_ids, got, wide[stream * width : (stream + 1) * width], scores[stream]
                )
                if step + 1 < TERMS:
                    xparts[stream] = column_parts(mine)
    total = jnp.concatenate(scores, axis=1)
    return jnp.swapaxes(total, 1, 2).reshape(BPD * tile, -1)


def solution(mesh):
    in_specs = (
        P("row", "col", None, None, None),
        P("row", "col", None),
        P("row", "col", None),
        P("row", "col"),
        P(),
        P(),
    )
    out_specs = P(("row", "col"), None)
    return jax.shard_map(shards, mesh=mesh, in_specs=in_specs, out_specs=out_specs, check_vma=False)
```

```python
import jax
import jax.numpy as jnp
from jax import lax
from jax.experimental import pallas as pl
from jax.experimental.pallas import tpu as pltpu
from jax.sharding import PartitionSpec as P

BPD = 8
TERMS = 4
TOUCH = 4
N_Z = 4
N_CORE = 2
STREAMS = 2
UNROLL = 8
CHUNK = 16
VMEM_LIMIT = 14 * 1024 * 1024

VMEM = pl.BlockSpec(memory_space=pltpu.VMEM)
HBM = pl.BlockSpec(memory_space=pltpu.HBM)
SMEM = pl.BlockSpec(memory_space=pltpu.SMEM)


def product_kernel(parts, turned, extra):
    def body(slot_ref, place_ref, count_ref, tiles_ref, *refs):
        x_refs, id_refs = refs[:parts], refs[parts:-5]
        out_ref, acc_ref, x_ref, tile_ref, sems = refs[-5:]
        count = count_ref[0]
        chunks = (count + CHUNK - 1) // CHUNK

        def chunk_copy(chunk):
            here = pl.ds(chunk * CHUNK, CHUNK)
            return pltpu.make_async_copy(tiles_ref.at[here], tile_ref.at[here], sems.at[chunk])

        def start(chunk, carry):
            chunk_copy(chunk).start()
            return carry

        lax.fori_loop(0, chunks, start, 0)
        each = x_ref.shape[0] // parts
        owners = out_ref.shape[0]
        width, tile = acc_ref.shape[1:]
        for part in range(parts):
            x_ref[part * each : (part + 1) * each] = x_refs[part][...]
        acc_ref[...] = jnp.zeros(acc_ref.shape, jnp.float32)

        def group(base):
            prods = []
            for lane in range(UNROLL):
                prods.append(
                    lax.dot_general(
                        x_ref[place_ref[base + lane]],
                        tile_ref[base + lane],
                        (((1,), (0 if turned else 1,)), ((), ())),
                        preferred_element_type=jnp.float32,
                    )
                )
            for lane in range(UNROLL):
                slot = slot_ref[base + lane]
                acc_ref[slot] = acc_ref[slot] + prods[lane]

        def chunk_step(chunk, carry):
            chunk_copy(chunk).wait()
            for part in range(CHUNK // UNROLL):
                group(chunk * CHUNK + part * UNROLL)
            return carry

        lax.fori_loop(0, chunks, chunk_step, 0)
        sent = acc_ref[: owners * TOUCH].astype(jnp.bfloat16).reshape(owners, TOUCH * width, tile)
        if extra:
            out_ref[:, : TOUCH * width] = sent
            out_ref[:, TOUCH * width :] = id_refs[0][...]
        else:
            out_ref[...] = sent

    return body


def products(slots, places, count, tiles, xparts, owners, turned, ids=()):
    parts = len(xparts)
    each, width, tile = xparts[0].shape
    extra = ids[0].shape[1] if ids else 0
    tiles = pltpu.with_memory_space_constraint(tiles, pltpu.HBM)
    return pl.pallas_call(
        product_kernel(parts, turned, extra),
        out_shape=jax.ShapeDtypeStruct((owners, TOUCH * width + extra, tile), jnp.bfloat16),
        in_specs=[SMEM, SMEM, SMEM, HBM] + [VMEM] * (parts + len(ids)),
        out_specs=VMEM,
        scratch_shapes=[
            pltpu.VMEM((owners * TOUCH + 1, width, tile), jnp.float32),
            pltpu.VMEM((parts * each, width, tile), jnp.bfloat16),
            pltpu.VMEM(tiles.shape, tiles.dtype),
            pltpu.SemaphoreType.DMA((tiles.shape[0] // CHUNK,)),
        ],
        compiler_params=pltpu.CompilerParams(vmem_limit_bytes=VMEM_LIMIT),
        name="products",
    )(slots, places, count, tiles, *xparts, *ids)


def turn_kernel(count_ref, tiles_ref, out_ref):
    def group(index, carry):
        for lane in range(UNROLL):
            out_ref[index * UNROLL + lane] = jnp.transpose(tiles_ref[index * UNROLL + lane])
        return carry

    lax.fori_loop(0, (count_ref[0] + UNROLL - 1) // UNROLL, group, 0)


def turned_tiles(count, tiles):
    return pl.pallas_call(
        turn_kernel,
        out_shape=jax.ShapeDtypeStruct(tiles.shape, tiles.dtype),
        in_specs=[SMEM, VMEM],
        out_specs=VMEM,
        compiler_params=pltpu.CompilerParams(vmem_limit_bytes=VMEM_LIMIT),
        name="turned",
    )(count, tiles)


def summed(id_ref, got_ref, acc_ref):
    width = acc_ref.shape[1]
    acc_ref[...] = jnp.zeros(acc_ref.shape, jnp.float32)
    for source in range(got_ref.shape[0]):
        for place in range(TOUCH):
            block = id_ref[source * TOUCH + place]
            part = got_ref[source, place * width : (place + 1) * width].astype(jnp.float32)
            acc_ref[block] = acc_ref[block] + part


def owned_kernel(step, first):
    def body(id_ref, got_ref, damping_ref, *refs):
        score_refs, (x_ref, out_ref, acc_ref) = refs[:-3], refs[-3:]
        summed(id_ref, got_ref, acc_ref)
        owned = acc_ref[: out_ref.shape[0]]
        x_ref[...] = owned.astype(jnp.bfloat16)
        if first:
            out_ref[...] = owned
        else:
            out_ref[...] = score_refs[0][...] + power(damping_ref, step)[None] * owned

    return body


def power(damping_ref, step):
    damping = damping_ref[...]
    coef = damping
    for _ in range(step - 1):
        coef = coef * damping
    return coef


def owned_sum(step, ids, got, damping, scores):
    shape = (BPD, *damping.shape)
    before = [] if step == 0 else [scores]
    return pl.pallas_call(
        owned_kernel(step, step == 0),
        out_shape=(
            jax.ShapeDtypeStruct(shape, jnp.bfloat16),
            jax.ShapeDtypeStruct(shape, jnp.float32),
        ),
        in_specs=[SMEM] + [VMEM] * (2 + len(before)),
        out_specs=(VMEM, VMEM),
        scratch_shapes=[pltpu.VMEM((BPD + 1, *damping.shape), jnp.float32)],
        compiler_params=pltpu.CompilerParams(vmem_limit_bytes=VMEM_LIMIT),
        name="owned",
    )(ids, got, damping, *before)


def last_kernel(step):
    def body(id_ref, got_ref, damping_ref, score_ref, done_ref, out_ref, acc_ref):
        summed(id_ref, got_ref, acc_ref)
        coef = power(damping_ref, step)
        for block in range(BPD):
            mine = score_ref[block] + coef * acc_ref[block]
            out_ref[block] = jnp.transpose(jnp.concatenate([done_ref[block], mine], axis=0))

    return body


def last_sum(step, ids, got, damping, scores, done):
    width, tile = damping.shape
    return pl.pallas_call(
        last_kernel(step),
        out_shape=jax.ShapeDtypeStruct((BPD, tile, done.shape[1] + width), jnp.float32),
        in_specs=[SMEM] + [VMEM] * 4,
        out_specs=VMEM,
        scratch_shapes=[pltpu.VMEM((BPD + 1, *damping.shape), jnp.float32)],
        compiler_params=pltpu.CompilerParams(vmem_limit_bytes=VMEM_LIMIT),
        name="last",
    )(ids, got, damping, scores, done)


def row_shift(dz, dcore):
    return [
        (z * N_CORE + core, (z + dz) % N_Z * N_CORE + (core + dcore) % N_CORE)
        for z in range(N_Z)
        for core in range(N_CORE)
    ]


def column_parts(mine):
    same = [mine] + [lax.ppermute(mine, "row", row_shift(dz, 0)) for dz in range(1, N_Z)]
    other = [lax.ppermute(part, "row", row_shift(0, 1)) for part in same]
    return same + other


def routes(rows, cols, count, n_col):
    slots = rows.shape[0]
    live = jnp.arange(slots, dtype=jnp.int32) < count
    blocks = jnp.arange(n_col * BPD, dtype=jnp.int32)
    hits = (rows[None, :] == blocks[:, None]) & live[None, :]
    marked = jnp.any(hits, axis=1).astype(jnp.int32).reshape(n_col, BPD)
    local = jnp.arange(BPD, dtype=jnp.int32)
    rank = jnp.sum(marked[:, None, :] * (local[None, None, :] < local[None, :, None]), axis=2)
    slot_of = (jnp.arange(n_col, dtype=jnp.int32)[:, None] * TOUCH + rank).reshape(-1)
    slot = jnp.sum(jnp.where(hits, slot_of[:, None], 0), axis=0)
    slot = jnp.where(live, slot, n_col * TOUCH)
    places = jnp.arange(TOUCH, dtype=jnp.int32)
    select = (marked[:, None, :] > 0) & (rank[:, None, :] == places[None, :, None])
    ids = jnp.sum(jnp.where(select, local[None, None, :] - BPD, 0), axis=2) + BPD
    row = lax.axis_index("row")
    owner, block = cols // BPD, cols % BPD
    far = (row // N_CORE - owner // N_CORE) % N_Z
    place = ((row % N_CORE != owner % N_CORE).astype(jnp.int32) * N_Z + far) * BPD + block
    return slot, place, ids


def shards(tiles, tile_row, tile_col, tile_count, query_ids, damping):
    tiles = tiles[0, 0]
    tile = tiles.shape[1]
    count = tile_count[0, 0]
    n_row, n_col = lax.axis_size("row"), lax.axis_size("col")
    slot, place, ids = routes(tile_row[0, 0], tile_col[0, 0], count, n_col)
    count = count.reshape(1)
    id_rows = jnp.pad(ids, ((0, 0), (0, 16 - TOUCH)), constant_values=BPD).astype(jnp.bfloat16)
    id_rows = jnp.broadcast_to(id_rows[:, :, None], (n_col, 16, tile))
    width = query_ids.shape[0] // STREAMS
    row, col = lax.axis_index("row"), lax.axis_index("col")
    part = jnp.arange(n_row * BPD, dtype=jnp.int32) // BPD
    core = (row + part // N_Z) % N_CORE
    z = (row // N_CORE - part) % N_Z
    block = ((z * N_CORE + core) * n_col + col) * BPD + jnp.arange(n_row * BPD, dtype=jnp.int32) % BPD
    nodes = block[:, None, None] * tile + jnp.arange(tile, dtype=jnp.int32)[None, None, :]
    xparts, dampings = [], []
    for stream in range(STREAMS):
        here = slice(stream * width, (stream + 1) * width)
        xparts.append([(nodes == query_ids[here][None, :, None]).astype(jnp.bfloat16)])
        dampings.append(jnp.broadcast_to(damping[here][:, None], (width, tile)))
    scores = [None] * STREAMS
    got_ids = turned = None
    for step in range(TERMS):
        for stream in range(STREAMS):
            with jax.named_scope(f"t{step}s{stream}"):
                first = step == 0 and stream == 0
                sent = products(
                    slot,
                    place,
                    count,
                    tiles if step == 0 else turned,
                    xparts[stream],
                    n_col,
                    step > 0,
                    (id_rows,) if first else (),
                )
                got = lax.all_to_all(sent, "col", split_axis=0, concat_axis=0, tiled=True)
                if first:
                    got_ids = got[:, -id_rows.shape[1] :, 0][:, :TOUCH].astype(jnp.int32).reshape(-1)
                if step == 0 and stream + 1 == STREAMS:
                    turned = turned_tiles(*lax.optimization_barrier((count, tiles, sent))[:2])
                args = (step, got_ids, got, dampings[stream], scores[stream])
                if step + 1 < TERMS:
                    mine, scores[stream] = owned_sum(*args)
                    xparts[stream] = column_parts(mine)
                elif stream + 1 < STREAMS:
                    scores[stream] = owned_sum(*args)[1]
                else:
                    total = last_sum(*args, *scores[:-1])
    return total.reshape(BPD * tile, -1)


def solution(mesh):
    in_specs = (
        P("row", "col", None, None, None),
        P("row", "col", None),
        P("row", "col", None),
        P("row", "col"),
        P(),
        P(),
    )
    out_specs = P(("row", "col"), None)
    return jax.shard_map(shards, mesh=mesh, in_specs=in_specs, out_specs=out_specs, check_vma=False)
```

```python
import jax
import jax.numpy as jnp
from jax import lax
from jax.experimental import pallas as pl
from jax.experimental.pallas import tpu as pltpu
from jax.sharding import PartitionSpec as P

BPD = 8
TERMS = 4
TOUCH = 4
N_Z = 4
N_CORE = 2
STREAMS = 2
PLACES = 32
ID_ROWS = 16
UNROLL = 8
CHUNK = 32
VMEM_LIMIT = 14 * 1024 * 1024

VMEM = pl.BlockSpec(memory_space=pltpu.VMEM)
HBM = pl.BlockSpec(memory_space=pltpu.HBM)
SMEM = pl.BlockSpec(memory_space=pltpu.SMEM)
PARAMS = pltpu.CompilerParams(vmem_limit_bytes=VMEM_LIMIT)
F32 = jnp.float32
BF16 = jnp.bfloat16


def power(damping_ref, step):
    damping = damping_ref[...]
    coef = damping
    for _ in range(step - 1):
        coef = coef * damping
    return coef


def multiply_tiles(slot_ref, place_ref, count, tiles_ref, x_parts, turned, acc_ref, x_ref, tile_ref, sems):
    chunks = (count + CHUNK - 1) // CHUNK

    def chunk_copy(chunk):
        here = pl.ds(chunk * CHUNK, CHUNK)
        return pltpu.make_async_copy(tiles_ref.at[here], tile_ref.at[here], sems.at[chunk])

    def start(chunk, carry):
        chunk_copy(chunk).start()
        return carry

    lax.fori_loop(0, chunks, start, 0)
    each = x_ref.shape[0] // len(x_parts)
    for part, part_ref in enumerate(x_parts):
        x_ref[part * each : (part + 1) * each] = part_ref[...]
    acc_ref[...] = jnp.zeros(acc_ref.shape, F32)

    def group(base):
        prods = []
        for lane in range(UNROLL):
            prods.append(
                lax.dot_general(
                    x_ref[place_ref[base + lane]],
                    tile_ref[base + lane],
                    (((1,), (0 if turned else 1,)), ((), ())),
                    preferred_element_type=F32,
                )
            )
        for lane in range(UNROLL):
            slot = slot_ref[base + lane]
            acc_ref[slot] = acc_ref[slot] + prods[lane]

    def chunk_step(chunk, carry):
        chunk_copy(chunk).wait()
        for part in range(CHUNK // UNROLL):
            group(chunk * CHUNK + part * UNROLL)
        return carry

    lax.fori_loop(0, chunks, chunk_step, 0)


def tile_scratch(sent, blocks, width, tiles):
    tile = tiles.shape[1]
    return [
        pltpu.VMEM((sent + 1, width, tile), F32),
        pltpu.VMEM((blocks, width, tile), BF16),
        pltpu.VMEM(tiles.shape, tiles.dtype),
        pltpu.SemaphoreType.DMA((tiles.shape[0] // CHUNK,)),
    ]


def first_products(slots, places, count, tiles, x, id_rows):
    owners, extra, tile = id_rows.shape
    blocks, width, _ = x.shape
    rows = TOUCH * width

    def body(slot_ref, place_ref, count_ref, tiles_ref, x_in, id_ref, out_ref, acc_ref, *scratch):
        multiply_tiles(slot_ref, place_ref, count_ref[0], tiles_ref, [x_in], False, acc_ref, *scratch)
        out_ref[:, :rows] = acc_ref[: owners * TOUCH].astype(BF16).reshape(owners, rows, tile)
        out_ref[:, rows:] = id_ref[...]

    return pl.pallas_call(
        body,
        out_shape=jax.ShapeDtypeStruct((owners, rows + extra, tile), BF16),
        in_specs=[SMEM, SMEM, SMEM, HBM, VMEM, VMEM],
        out_specs=VMEM,
        scratch_shapes=tile_scratch(owners * TOUCH, blocks, width, tiles),
        compiler_params=PARAMS,
        name="first_products",
    )(slots, places, count, pltpu.with_memory_space_constraint(tiles, pltpu.HBM), x, id_rows)


def products(step, slots, places, count, turned, xparts, owners, damping, owned, scores):
    parts = len(xparts)
    each, width, tile = xparts[0].shape
    rows = TOUCH * width
    before = [] if step == 1 else [scores]

    def body(slot_ref, place_ref, count_ref, tiles_ref, *refs):
        x_refs, (damping_ref, owned_ref), refs = refs[:parts], refs[parts : parts + 2], refs[parts + 2 :]
        score_in, refs = refs[: len(before)], refs[len(before) :]
        out_ref, score_out, score_ref, score_sems, acc_ref, *scratch = refs
        for ref in score_in:
            pltpu.make_async_copy(ref, score_ref, score_sems.at[0]).start()
        multiply_tiles(slot_ref, place_ref, count_ref[0], tiles_ref, x_refs, True, acc_ref, *scratch)
        for ref in score_in:
            pltpu.make_async_copy(ref, score_ref, score_sems.at[0]).wait()
        if score_in:
            score_ref[...] = score_ref[...] + power(damping_ref, step - 1)[None] * owned_ref[...]
        else:
            score_ref[...] = owned_ref[...]
        leave = pltpu.make_async_copy(score_ref, score_out, score_sems.at[1])
        leave.start()
        out_ref[...] = acc_ref[: owners * TOUCH].astype(BF16).reshape(owners, rows, tile)
        leave.wait()

    return pl.pallas_call(
        body,
        out_shape=(
            jax.ShapeDtypeStruct((owners, rows, tile), BF16),
            pltpu.HBM((BPD, width, tile), F32),
        ),
        in_specs=[SMEM, SMEM, SMEM, HBM] + [VMEM] * (parts + 2) + [HBM] * len(before),
        out_specs=(VMEM, HBM),
        scratch_shapes=[
            pltpu.VMEM((BPD, width, tile), F32),
            pltpu.SemaphoreType.DMA((2,)),
            *tile_scratch(owners * TOUCH, parts * each, width, turned),
        ],
        compiler_params=PARAMS,
        name="products",
    )(
        slots,
        places,
        count,
        pltpu.with_memory_space_constraint(turned, pltpu.HBM),
        *xparts,
        damping,
        owned,
        *[pltpu.with_memory_space_constraint(part, pltpu.HBM) for part in before],
    )


def turned_tiles(count, tiles):
    def body(count_ref, tiles_ref, out_ref):
        def group(index, carry):
            for lane in range(UNROLL):
                out_ref[index * UNROLL + lane] = jnp.transpose(tiles_ref[index * UNROLL + lane])
            return carry

        lax.fori_loop(0, (count_ref[0] + UNROLL - 1) // UNROLL, group, 0)

    return pl.pallas_call(
        body,
        out_shape=jax.ShapeDtypeStruct(tiles.shape, tiles.dtype),
        in_specs=[SMEM, VMEM],
        out_specs=VMEM,
        compiler_params=PARAMS,
        name="turned",
    )(count, tiles)


def summed(id_ref, got_ref, acc_ref):
    width = acc_ref.shape[1]
    acc_ref[...] = jnp.zeros(acc_ref.shape, F32)
    for source in range(got_ref.shape[0]):
        for place in range(TOUCH):
            block = id_ref[source * TOUCH + place]
            part = got_ref[source, place * width : (place + 1) * width].astype(F32)
            acc_ref[block] = acc_ref[block] + part


def owned_sum(ids, got, damping):
    width, tile = damping.shape

    def body(id_ref, got_ref, x_ref, out_ref, acc_ref):
        summed(id_ref, got_ref, acc_ref)
        owned = acc_ref[:BPD]
        x_ref[...] = owned.astype(BF16)
        out_ref[...] = owned

    return pl.pallas_call(
        body,
        out_shape=(
            jax.ShapeDtypeStruct((BPD, width, tile), BF16),
            jax.ShapeDtypeStruct((BPD, width, tile), F32),
        ),
        in_specs=[SMEM, VMEM],
        out_specs=(VMEM, VMEM),
        scratch_shapes=[pltpu.VMEM((BPD + 1, width, tile), F32)],
        compiler_params=PARAMS,
        name="owned",
    )(ids, got)


def placed_sum(ids, got, spread, width):
    sources, _, tile = got.shape
    queries, columns = spread.shape
    streams = queries // width

    def body(id_ref, got_ref, spread_ref, *refs):
        x_refs, out_refs, piece_ref = refs[:streams], refs[streams : 2 * streams], refs[-1]
        piece_ref[...] = jnp.zeros(piece_ref.shape, BF16)
        for source in range(sources):
            for place in range(TOUCH):
                block = id_ref[source * TOUCH + place]
                piece_ref[block, source * PLACES : (source + 1) * PLACES] = got_ref[
                    source, place * PLACES : (place + 1) * PLACES
                ]
        for block in range(BPD):
            owned = jnp.dot(spread_ref[...], piece_ref[block], preferred_element_type=F32)
            for stream in range(streams):
                mine = owned[stream * width : (stream + 1) * width]
                x_refs[stream][block] = mine.astype(BF16)
                out_refs[stream][block] = mine

    shape = (BPD, width, tile)
    return pl.pallas_call(
        body,
        out_shape=[jax.ShapeDtypeStruct(shape, BF16)] * streams + [jax.ShapeDtypeStruct(shape, F32)] * streams,
        in_specs=[SMEM, VMEM, VMEM],
        out_specs=[VMEM] * (2 * streams),
        scratch_shapes=[pltpu.VMEM((BPD + 1, columns, tile), BF16)],
        compiler_params=PARAMS,
        name="placed",
    )(ids, got, spread)


def ended_sum(step, ids, got, damping, scores):
    width, tile = damping.shape

    def body(id_ref, got_ref, damping_ref, score_ref, out_ref, acc_ref):
        summed(id_ref, got_ref, acc_ref)
        out_ref[...] = score_ref[...] + power(damping_ref, step)[None] * acc_ref[:BPD]

    return pl.pallas_call(
        body,
        out_shape=jax.ShapeDtypeStruct((BPD, width, tile), F32),
        in_specs=[SMEM] + [VMEM] * 3,
        out_specs=VMEM,
        scratch_shapes=[pltpu.VMEM((BPD + 1, width, tile), F32)],
        compiler_params=PARAMS,
        name="ended",
    )(ids, got, damping, scores)


def last_sum(step, ids, got, damping, scores, *done):
    width, tile = damping.shape
    queries = sum(part.shape[1] for part in done) + width

    def body(id_ref, got_ref, damping_ref, score_ref, *refs):
        done_refs, (out_ref, acc_ref) = refs[:-2], refs[-2:]
        summed(id_ref, got_ref, acc_ref)
        coef = power(damping_ref, step)
        for block in range(BPD):
            mine = score_ref[block] + coef * acc_ref[block]
            rows = [part[block] for part in done_refs] + [mine]
            out_ref[block] = jnp.transpose(jnp.concatenate(rows, axis=0))

    return pl.pallas_call(
        body,
        out_shape=jax.ShapeDtypeStruct((BPD, tile, queries), F32),
        in_specs=[SMEM] + [VMEM] * (3 + len(done)),
        out_specs=VMEM,
        scratch_shapes=[pltpu.VMEM((BPD + 1, width, tile), F32)],
        compiler_params=PARAMS,
        name="last",
    )(ids, got, damping, scores, *done)


def row_shift(dz, dcore):
    return [
        (z * N_CORE + core, (z + dz) % N_Z * N_CORE + (core + dcore) % N_CORE)
        for z in range(N_Z)
        for core in range(N_CORE)
    ]


def column_parts(mine):
    same = [mine] + [lax.ppermute(mine, "row", row_shift(dz, 0)) for dz in range(1, N_Z)]
    other = [lax.ppermute(part, "row", row_shift(0, 1)) for part in same]
    return same + other


def after(value, *others):
    return lax.optimization_barrier((value, *others))[0]


def exchange(sent):
    return lax.all_to_all(sent, "col", split_axis=0, concat_axis=0, tiled=True)


def routes(rows, cols, count, n_col):
    slots = rows.shape[0]
    live = jnp.arange(slots, dtype=jnp.int32) < count
    blocks = jnp.arange(n_col * BPD, dtype=jnp.int32)
    hits = (rows[None, :] == blocks[:, None]) & live[None, :]
    marked = jnp.any(hits, axis=1).astype(jnp.int32).reshape(n_col, BPD)
    local = jnp.arange(BPD, dtype=jnp.int32)
    rank = jnp.sum(marked[:, None, :] * (local[None, None, :] < local[None, :, None]), axis=2)
    slot_of = (jnp.arange(n_col, dtype=jnp.int32)[:, None] * TOUCH + rank).reshape(-1)
    slot = jnp.sum(jnp.where(hits, slot_of[:, None], 0), axis=0)
    slot = jnp.where(live, slot, n_col * TOUCH)
    places = jnp.arange(TOUCH, dtype=jnp.int32)
    select = (marked[:, None, :] > 0) & (rank[:, None, :] == places[None, :, None])
    ids = jnp.sum(jnp.where(select, local[None, None, :] - BPD, 0), axis=2) + BPD
    row = lax.axis_index("row")
    owner, block = cols // BPD, cols % BPD
    far = (row // N_CORE - owner // N_CORE) % N_Z
    place = ((row % N_CORE != owner % N_CORE).astype(jnp.int32) * N_Z + far) * BPD + block
    return slot, place, ids


def shards(tiles, tile_row, tile_col, tile_count, query_ids, damping):
    tiles = tiles[0, 0]
    tile = tiles.shape[1]
    count = tile_count[0, 0]
    queries = query_ids.shape[0]
    n_row, n_col = lax.axis_size("row"), lax.axis_size("col")
    row, col = lax.axis_index("row"), lax.axis_index("col")
    slot, place, ids = routes(tile_row[0, 0], tile_col[0, 0], count, n_col)
    count = count.reshape(1)
    id_rows = jnp.pad(ids, ((0, 0), (0, ID_ROWS - TOUCH)), constant_values=BPD).astype(BF16)
    id_rows = jnp.broadcast_to(id_rows[:, :, None], (n_col, ID_ROWS, tile))
    width = queries // STREAMS
    part = jnp.arange(n_row * BPD, dtype=jnp.int32) // BPD
    core = (row + part // N_Z) % N_CORE
    z = (row // N_CORE - part) % N_Z
    block = ((z * N_CORE + core) * n_col + col) * BPD + jnp.arange(n_row * BPD, dtype=jnp.int32) % BPD
    nodes = block[:, None, None] * tile + jnp.arange(tile, dtype=jnp.int32)[None, None, :]
    dampings = [
        jnp.broadcast_to(damping[stream * width : (stream + 1) * width][:, None], (width, tile))
        for stream in range(STREAMS)
    ]

    home = query_ids // (BPD * tile) % n_col
    number = jnp.arange(queries, dtype=jnp.int32)
    same_home = home[:, None] == home[None, :]
    rank = jnp.sum((same_home & (number[None, :] < number[:, None])).astype(jnp.int32), axis=1)
    fits = jnp.all(rank < PLACES)

    def sent_ids(got):
        return got[:, -ID_ROWS:, 0][:, :TOUCH].astype(jnp.int32).reshape(-1)

    def own_queries():
        lane = jnp.arange(PLACES, dtype=jnp.int32)
        here = (home == col)[None, :] & (rank[None, :] == lane[:, None])
        asked = jnp.sum(jnp.where(here, query_ids[None, :] + 1, 0), axis=1) - 1
        x = (nodes == asked[None, :, None]).astype(BF16)
        column = home * PLACES + rank
        spread = (column[:, None] == jnp.arange(n_col * PLACES, dtype=jnp.int32)[None, :]).astype(BF16)
        sent = first_products(slot, place, count, tiles, x, id_rows)
        got = exchange(sent)
        turned = turned_tiles(count, after(tiles, sent))
        got_ids = sent_ids(got)
        owned = placed_sum(got_ids, after(got, turned), spread, width)
        return (*owned, got_ids, turned)

    def all_queries():
        rounded, whole = [], []
        for stream in range(STREAMS):
            asked = query_ids[stream * width : (stream + 1) * width]
            x = (nodes == asked[None, :, None]).astype(BF16)
            got = exchange(first_products(slot, place, count, tiles, x, id_rows))
            got_ids = sent_ids(got)
            mine = owned_sum(got_ids, got, dampings[stream])
            rounded.append(mine[0])
            whole.append(mine[1])
        return (*rounded, *whole, got_ids, turned_tiles(count, tiles))

    *sums, got_ids, turned = lax.cond(fits, own_queries, all_queries)
    xparts = [column_parts(sums[stream]) for stream in range(STREAMS)]
    owned, scores = sums[STREAMS:], [None] * STREAMS
    for step in range(1, TERMS):
        for stream in range(STREAMS):
            with jax.named_scope(f"t{step}s{stream}"):
                sent, scores[stream] = products(
                    step,
                    slot,
                    place,
                    count,
                    turned,
                    xparts[stream],
                    n_col,
                    dampings[stream],
                    owned[stream],
                    scores[stream],
                )
                got = exchange(sent)
                if step + 1 < TERMS:
                    mine, owned[stream] = owned_sum(got_ids, got, dampings[stream])
                    xparts[stream] = column_parts(mine)
                elif stream + 1 < STREAMS:
                    scores[stream] = ended_sum(step, got_ids, got, dampings[stream], scores[stream])
                else:
                    total = last_sum(step, got_ids, got, dampings[stream], scores[stream], *scores[:-1])
    return total.reshape(BPD * tile, -1)


def solution(mesh):
    in_specs = (
        P("row", "col", None, None, None),
        P("row", "col", None),
        P("row", "col", None),
        P("row", "col"),
        P(),
        P(),
    )
    out_specs = P(("row", "col"), None)
    return jax.shard_map(shards, mesh=mesh, in_specs=in_specs, out_specs=out_specs, check_vma=False)
```

```python
import jax
import jax.numpy as jnp
from jax import lax
from jax.experimental import pallas as pl
from jax.experimental.pallas import tpu as pltpu
from jax.sharding import PartitionSpec as P


BPD = 8
TERMS = 4
TOUCH = 4
N_Z = 4
N_CORE = 2
STREAMS = 2
PLACES = 32
ID_ROWS = 16
UNROLL = 8
FIRST_UNROLL = 4
CHUNK = 32
VMEM_LIMIT = 14 * 1024 * 1024

VMEM = pl.BlockSpec(memory_space=pltpu.VMEM)
HBM = pl.BlockSpec(memory_space=pltpu.HBM)
SMEM = pl.BlockSpec(memory_space=pltpu.SMEM)
PARAMS = pltpu.CompilerParams(vmem_limit_bytes=VMEM_LIMIT)
F32 = jnp.float32
BF16 = jnp.bfloat16


def power(damping_ref, step):
    damping = damping_ref[...]
    coef = damping
    for _ in range(step - 1):
        coef = coef * damping
    return coef


def multiply_tiles(slot_ref, place_ref, count, tiles_ref, x_parts, turned, acc_ref, x_ref, tile_ref, sems):
    chunks = (count + CHUNK - 1) // CHUNK

    def chunk_copy(chunk):
        here = pl.ds(chunk * CHUNK, CHUNK)
        return pltpu.make_async_copy(tiles_ref.at[here], tile_ref.at[here], sems.at[chunk])

    def start(chunk, carry):
        chunk_copy(chunk).start()
        return carry

    lax.fori_loop(0, chunks, start, 0)
    each = x_ref.shape[0] // len(x_parts)
    for part, part_ref in enumerate(x_parts):
        x_ref[part * each : (part + 1) * each] = part_ref[...]
    acc_ref[...] = jnp.zeros(acc_ref.shape, F32)

    def group(base):
        prods = []
        for lane in range(UNROLL):
            prods.append(
                lax.dot_general(
                    x_ref[place_ref[base + lane]],
                    tile_ref[base + lane],
                    (((1,), (0 if turned else 1,)), ((), ())),
                    preferred_element_type=F32,
                )
            )
        for lane in range(UNROLL):
            slot = slot_ref[base + lane]
            acc_ref[slot] = acc_ref[slot] + prods[lane]

    def chunk_step(chunk, carry):
        chunk_copy(chunk).wait()
        for part in range(CHUNK // UNROLL):
            group(chunk * CHUNK + part * UNROLL)
        return carry

    lax.fori_loop(0, chunks, chunk_step, 0)


def tile_scratch(sent, blocks, width, tiles):
    tile = tiles.shape[1]
    return [
        pltpu.VMEM((sent + 1, width, tile), F32),
        pltpu.VMEM((blocks, width, tile), BF16),
        pltpu.VMEM(tiles.shape, tiles.dtype),
        pltpu.SemaphoreType.DMA((tiles.shape[0] // CHUNK,)),
    ]


def first_products(round_index, rows, cols, query_ids, count, col, tiles, n_col, n_row):
    slots, tile, _ = tiles.shape
    queries = query_ids.shape[0]
    col_blocks = n_row * BPD
    row_blocks = n_col * BPD
    spare = n_col * TOUCH
    sent_rows = TOUCH * PLACES
    tile_bits, col_bits, block_bits = (n.bit_length() - 1 for n in (tile, n_col, BPD))

    def body(info_ref, row_ref, col_ref, query_ref, tiles_ref, out_ref, *scratch):
        acc_ref, x_ref, tile_ref, id_rows_ref, asked_ref, has_ref, list_ref, mark_ref, slot_ref, id_ref, sems = scratch
        live, mine, first = info_ref[0], info_ref[1], info_ref[2] * PLACES

        def repeat(times, step, start=0, unroll=8):
            return lax.fori_loop(0, times, step, start, unroll=unroll)

        def clear(ref, value):
            def step(index, carry):
                ref[index] = value
                return carry

            repeat(ref.shape[0], step)

        def copy(index, lane):
            return pltpu.make_async_copy(tiles_ref.at[index], tile_ref.at[lane], sems.at[lane])

        def ask(query, found):
            node = query_ref[query]
            asked_ref[found] = node
            home = (node >> (tile_bits + block_bits)) & (n_col - 1)
            return found + (home == mine).astype(jnp.int32)

        asked = repeat(queries, ask)
        clear(has_ref, 0)
        x_ref[...] = jnp.zeros(x_ref.shape, BF16)
        place_of = lax.broadcasted_iota(jnp.int32, (PLACES, tile), 0)
        node_of = lax.broadcasted_iota(jnp.int32, (PLACES, tile), 1)

        def mark_query(place, carry):
            node = asked_ref[first + place]
            block = (node >> (tile_bits + block_bits + col_bits)) * BPD + ((node >> tile_bits) & (BPD - 1))
            here = (place_of == place) & (node_of == (node & (tile - 1)))
            x_ref[block] = jnp.where(here, 1.0, x_ref[block].astype(F32)).astype(BF16)
            has_ref[block] = 1
            return carry

        lax.fori_loop(0, jnp.clip(asked - first, 0, PLACES), mark_query, 0)

        def pick(index, found):
            list_ref[found] = index
            return found + jnp.where(index < live, has_ref[col_ref[index]], 0)

        found = repeat(slots, pick)

        def start(lane, carry):
            copy(list_ref[lane], lane).start()
            return carry

        lax.fori_loop(0, found, start, 0)
        clear(mark_ref, 0)

        def mark_row(index, carry):
            mark_ref[jnp.where(index < live, row_ref[index], row_blocks)] = 1
            return carry

        repeat(slots, mark_row)
        clear(id_ref, BPD)
        id_rows_ref[...] = jnp.full(id_rows_ref.shape, float(BPD), F32)

        def number_owner(owner, carry):
            rank = 0
            for block in range(BPD):
                marked = mark_ref[owner * BPD + block]
                slot_ref[owner * BPD + block] = owner * TOUCH + rank
                id_ref[owner * TOUCH + rank] = jnp.where(marked > 0, block, BPD)
                rank = rank + marked
            for place in range(TOUCH):
                number = id_ref[owner * TOUCH + place].astype(F32)
                id_rows_ref[owner, place : place + 1] = jnp.full((1, tile), number, F32)
            return carry

        repeat(n_col, number_owner, unroll=1)
        acc_ref[...] = jnp.zeros(acc_ref.shape, F32)

        def step(index, carry):
            prods, goes = [], []
            for lane in range(FIRST_UNROLL):
                at = index * FIRST_UNROLL + lane
                valid = at < found
                which = jnp.where(valid, list_ref[at], 0)

                @pl.when(valid)
                def _():
                    copy(which, at).wait()

                goes.append((at, which, valid))
            for at, which, valid in goes:
                prods.append(
                    lax.dot_general(
                        x_ref[col_ref[which]], tile_ref[at], (((1,), (1,)), ((), ())), preferred_element_type=F32
                    )
                )
            for (at, which, valid), prod in zip(goes, prods):
                slot = jnp.where(valid, slot_ref[row_ref[which]], spare)
                acc_ref[slot] = acc_ref[slot] + prod
            return carry

        lax.fori_loop(0, (found + FIRST_UNROLL - 1) // FIRST_UNROLL, step, 0)
        out_ref[:, :sent_rows] = acc_ref[:spare].astype(BF16).reshape(n_col, sent_rows, tile)
        out_ref[:, sent_rows:] = id_rows_ref[...].astype(BF16)

    info = jnp.stack([count, col, round_index]).astype(jnp.int32)
    return pl.pallas_call(
        body,
        out_shape=jax.ShapeDtypeStruct((n_col, sent_rows + ID_ROWS, tile), BF16),
        in_specs=[SMEM, SMEM, SMEM, SMEM, HBM],
        out_specs=VMEM,
        scratch_shapes=[
            pltpu.VMEM((spare + 1, PLACES, tile), F32),
            pltpu.VMEM((col_blocks, PLACES, tile), BF16),
            pltpu.VMEM(tiles.shape, tiles.dtype),
            pltpu.VMEM((n_col, ID_ROWS, tile), F32),
            pltpu.SMEM((queries,), jnp.int32),
            pltpu.SMEM((col_blocks,), jnp.int32),
            pltpu.SMEM((slots,), jnp.int32),
            pltpu.SMEM((row_blocks + 8,), jnp.int32),
            pltpu.SMEM((row_blocks,), jnp.int32),
            pltpu.SMEM((spare + 8,), jnp.int32),
            pltpu.SemaphoreType.DMA((slots,)),
        ],
        compiler_params=PARAMS,
        name="first_products",
    )(info, rows, cols, query_ids, pltpu.with_memory_space_constraint(tiles, pltpu.HBM))


def products(step, slots, places, count, turned, xparts, owners, damping, owned, scores):
    parts = len(xparts)
    each, width, tile = xparts[0].shape
    rows = TOUCH * width
    before = [] if step == 1 else [scores]

    def body(slot_ref, place_ref, count_ref, tiles_ref, *refs):
        x_refs, (damping_ref, owned_ref), refs = refs[:parts], refs[parts : parts + 2], refs[parts + 2 :]
        score_in, refs = refs[: len(before)], refs[len(before) :]
        out_ref, score_out, score_ref, score_sems, acc_ref, *scratch = refs
        for ref in score_in:
            pltpu.make_async_copy(ref, score_ref, score_sems.at[0]).start()
        multiply_tiles(slot_ref, place_ref, count_ref[0], tiles_ref, x_refs, True, acc_ref, *scratch)
        for ref in score_in:
            pltpu.make_async_copy(ref, score_ref, score_sems.at[0]).wait()
        if score_in:
            score_ref[...] = score_ref[...] + power(damping_ref, step - 1)[None] * owned_ref[...]
        else:
            score_ref[...] = owned_ref[...]
        leave = pltpu.make_async_copy(score_ref, score_out, score_sems.at[1])
        leave.start()
        out_ref[...] = acc_ref[: owners * TOUCH].astype(BF16).reshape(owners, rows, tile)
        leave.wait()

    return pl.pallas_call(
        body,
        out_shape=(
            jax.ShapeDtypeStruct((owners, rows, tile), BF16),
            pltpu.HBM((BPD, width, tile), F32),
        ),
        in_specs=[SMEM, SMEM, SMEM, HBM] + [VMEM] * (parts + 2) + [HBM] * len(before),
        out_specs=(VMEM, HBM),
        scratch_shapes=[
            pltpu.VMEM((BPD, width, tile), F32),
            pltpu.SemaphoreType.DMA((2,)),
            *tile_scratch(owners * TOUCH, parts * each, width, turned),
        ],
        compiler_params=PARAMS,
        name="products",
    )(
        slots,
        places,
        count,
        pltpu.with_memory_space_constraint(turned, pltpu.HBM),
        *xparts,
        damping,
        owned,
        *[pltpu.with_memory_space_constraint(part, pltpu.HBM) for part in before],
    )


def turned_tiles(count, tiles):
    def body(count_ref, tiles_ref, out_ref):
        def group(index, carry):
            for lane in range(UNROLL):
                out_ref[index * UNROLL + lane] = jnp.transpose(tiles_ref[index * UNROLL + lane])
            return carry

        lax.fori_loop(0, (count_ref[0] + UNROLL - 1) // UNROLL, group, 0)

    return pl.pallas_call(
        body,
        out_shape=jax.ShapeDtypeStruct(tiles.shape, tiles.dtype),
        in_specs=[SMEM, VMEM],
        out_specs=VMEM,
        compiler_params=PARAMS,
        name="turned",
    )(count, tiles)


def summed(id_ref, got_ref, acc_ref):
    width = acc_ref.shape[1]
    acc_ref[...] = jnp.zeros(acc_ref.shape, F32)
    for source in range(got_ref.shape[0]):
        for place in range(TOUCH):
            block = id_ref[source * TOUCH + place]
            part = got_ref[source, place * width : (place + 1) * width].astype(F32)
            acc_ref[block] = acc_ref[block] + part


def owned_sum(ids, got, damping):
    width, tile = damping.shape

    def body(id_ref, got_ref, x_ref, out_ref, acc_ref):
        summed(id_ref, got_ref, acc_ref)
        owned = acc_ref[:BPD]
        x_ref[...] = owned.astype(BF16)
        out_ref[...] = owned

    return pl.pallas_call(
        body,
        out_shape=(
            jax.ShapeDtypeStruct((BPD, width, tile), BF16),
            jax.ShapeDtypeStruct((BPD, width, tile), F32),
        ),
        in_specs=[SMEM, VMEM],
        out_specs=(VMEM, VMEM),
        scratch_shapes=[pltpu.VMEM((BPD + 1, width, tile), F32)],
        compiler_params=PARAMS,
        name="owned",
    )(ids, got)


def placed_sum(ids, got, spread, width, before=()):
    sources, _, tile = got.shape
    queries, columns = spread.shape
    streams = queries // width

    def body(id_ref, got_ref, spread_ref, *refs):
        whole_refs, refs = refs[: len(before)], refs[len(before) :]
        x_refs, out_refs, piece_ref = refs[:streams], refs[streams : 2 * streams], refs[-1]
        piece_ref[...] = jnp.zeros(piece_ref.shape, BF16)
        for source in range(sources):
            for place in range(TOUCH):
                block = id_ref[source * TOUCH + place]
                piece_ref[block, source * PLACES : (source + 1) * PLACES] = got_ref[
                    source, place * PLACES : (place + 1) * PLACES
                ]
        for block in range(BPD):
            owned = jnp.dot(spread_ref[...], piece_ref[block], preferred_element_type=F32)
            for stream in range(streams):
                mine = owned[stream * width : (stream + 1) * width]
                if whole_refs:
                    mine = mine + whole_refs[stream][block]
                x_refs[stream][block] = mine.astype(BF16)
                out_refs[stream][block] = mine

    shape = (BPD, width, tile)
    return pl.pallas_call(
        body,
        out_shape=[jax.ShapeDtypeStruct(shape, BF16)] * streams + [jax.ShapeDtypeStruct(shape, F32)] * streams,
        in_specs=[SMEM] + [VMEM] * (2 + len(before)),
        out_specs=[VMEM] * (2 * streams),
        scratch_shapes=[pltpu.VMEM((BPD + 1, columns, tile), BF16)],
        compiler_params=PARAMS,
        name="placed",
    )(ids, got, spread, *before)


def ended_sum(step, ids, got, damping, scores):
    width, tile = damping.shape

    def body(id_ref, got_ref, damping_ref, score_ref, out_ref, acc_ref):
        summed(id_ref, got_ref, acc_ref)
        out_ref[...] = score_ref[...] + power(damping_ref, step)[None] * acc_ref[:BPD]

    return pl.pallas_call(
        body,
        out_shape=jax.ShapeDtypeStruct((BPD, width, tile), F32),
        in_specs=[SMEM] + [VMEM] * 3,
        out_specs=VMEM,
        scratch_shapes=[pltpu.VMEM((BPD + 1, width, tile), F32)],
        compiler_params=PARAMS,
        name="ended",
    )(ids, got, damping, scores)


def last_sum(step, ids, got, damping, scores, *done):
    width, tile = damping.shape
    queries = sum(part.shape[1] for part in done) + width

    def body(id_ref, got_ref, damping_ref, score_ref, *refs):
        done_refs, (out_ref, acc_ref) = refs[:-2], refs[-2:]
        summed(id_ref, got_ref, acc_ref)
        coef = power(damping_ref, step)
        for block in range(BPD):
            mine = score_ref[block] + coef * acc_ref[block]
            rows = [part[block] for part in done_refs] + [mine]
            out_ref[block] = jnp.transpose(jnp.concatenate(rows, axis=0))

    return pl.pallas_call(
        body,
        out_shape=jax.ShapeDtypeStruct((BPD, tile, queries), F32),
        in_specs=[SMEM] + [VMEM] * (3 + len(done)),
        out_specs=VMEM,
        scratch_shapes=[pltpu.VMEM((BPD + 1, width, tile), F32)],
        compiler_params=PARAMS,
        name="last",
    )(ids, got, damping, scores, *done)


def row_shift(dz, dcore):
    return [
        (z * N_CORE + core, (z + dz) % N_Z * N_CORE + (core + dcore) % N_CORE)
        for z in range(N_Z)
        for core in range(N_CORE)
    ]


def column_parts(mine):
    same = [mine] + [lax.ppermute(mine, "row", row_shift(dz, 0)) for dz in range(1, N_Z)]
    other = [lax.ppermute(part, "row", row_shift(0, 1)) for part in same]
    return same + other


def after(value, *others):
    return lax.optimization_barrier((value, *others))[0]


def exchange(sent):
    return lax.all_to_all(sent, "col", split_axis=0, concat_axis=0, tiled=True)


def routes(rows, cols, count, n_col):
    slots = rows.shape[0]
    live = jnp.arange(slots, dtype=jnp.int32) < count
    blocks = jnp.arange(n_col * BPD, dtype=jnp.int32)
    hits = (rows[None, :] == blocks[:, None]) & live[None, :]
    marked = jnp.any(hits, axis=1).astype(jnp.int32).reshape(n_col, BPD)
    local = jnp.arange(BPD, dtype=jnp.int32)
    rank = jnp.sum(marked[:, None, :] * (local[None, None, :] < local[None, :, None]), axis=2)
    slot_of = (jnp.arange(n_col, dtype=jnp.int32)[:, None] * TOUCH + rank).reshape(-1)
    slot = jnp.sum(jnp.where(hits, slot_of[:, None], 0), axis=0)
    slot = jnp.where(live, slot, n_col * TOUCH)
    row = lax.axis_index("row")
    owner, block = cols // BPD, cols % BPD
    far = (row // N_CORE - owner // N_CORE) % N_Z
    place = ((row % N_CORE != owner % N_CORE).astype(jnp.int32) * N_Z + far) * BPD + block
    return slot, place


def shards(tiles, tile_row, tile_col, tile_count, query_ids, damping):
    tiles, rows, cols, count = tiles[0, 0], tile_row[0, 0], tile_col[0, 0], tile_count[0, 0]
    tile = tiles.shape[1]
    queries = query_ids.shape[0]
    width = queries // STREAMS
    n_row, n_col = lax.axis_size("row"), lax.axis_size("col")
    col = lax.axis_index("col")

    def first_sent(round_index):
        return first_products(round_index, rows, cols, query_ids, count, col, tiles, n_col, n_row)

    sent = first_sent(0)
    got = exchange(sent)

    later_ids = after(query_ids, sent)
    home = later_ids // (BPD * tile) % n_col
    number = jnp.arange(queries, dtype=jnp.int32)
    same_home = home[:, None] == home[None, :]
    rank = jnp.sum((same_home & (number[None, :] < number[:, None])).astype(jnp.int32), axis=1)
    rounds = jnp.max(rank) // PLACES + 1

    def spread(round_index):
        place = rank - round_index * PLACES
        column = jnp.where((place >= 0) & (place < PLACES), home * PLACES + place, -1)
        return (column[:, None] == jnp.arange(n_col * PLACES, dtype=jnp.int32)[None, :]).astype(BF16)

    slot, place = routes(after(rows, sent), cols, count, n_col)
    turned = turned_tiles(count.reshape(1), after(tiles, sent))
    first_spread = spread(0)
    got_ids = got[:, -ID_ROWS:, 0][:, :TOUCH].astype(jnp.int32).reshape(-1)
    sums = placed_sum(got_ids, after(got, turned, slot, place, first_spread), first_spread, width)

    def next_round(state):
        index, *sums = state
        got = exchange(first_sent(index))
        return index + 1, *placed_sum(got_ids, got, spread(index), width, sums[STREAMS:])

    _, *sums = lax.while_loop(lambda state: state[0] < rounds, next_round, (jnp.int32(1), *sums))
    count = count.reshape(1)
    dampings = [
        jnp.broadcast_to(damping[stream * width : (stream + 1) * width][:, None], (width, tile))
        for stream in range(STREAMS)
    ]
    xparts = [column_parts(sums[stream]) for stream in range(STREAMS)]
    owned, scores = sums[STREAMS:], [None] * STREAMS
    for step in range(1, TERMS):
        for stream in range(STREAMS):
            sent, scores[stream] = products(
                step,
                slot,
                place,
                count,
                turned,
                xparts[stream],
                n_col,
                dampings[stream],
                owned[stream],
                scores[stream],
            )
            got = exchange(sent)
            if step + 1 < TERMS:
                mine, owned[stream] = owned_sum(got_ids, got, dampings[stream])
                xparts[stream] = column_parts(mine)
            elif stream + 1 < STREAMS:
                scores[stream] = ended_sum(step, got_ids, got, dampings[stream], scores[stream])
            else:
                total = last_sum(step, got_ids, got, dampings[stream], scores[stream], *scores[:-1])
    return total.reshape(BPD * tile, -1)


def solution(mesh):
    in_specs = (
        P("row", "col", None, None, None),
        P("row", "col", None),
        P("row", "col", None),
        P("row", "col"),
        P(),
        P(),
    )
    out_specs = P(("row", "col"), None)
    return jax.shard_map(shards, mesh=mesh, in_specs=in_specs, out_specs=out_specs, check_vma=False)
```

```python
import jax
import jax.numpy as jnp
from jax import lax
from jax.experimental import pallas as pl
from jax.experimental.pallas import tpu as pltpu
from jax.sharding import PartitionSpec as P


BPD = 8
TERMS = 4
TOUCH = 4
N_Z = 4
N_CORE = 2
STREAMS = 2
PLACES = 32
ID_ROWS = 16
UNROLL = 8
FIRST_UNROLL = 4
CHUNK = 32
VMEM_LIMIT = 14 * 1024 * 1024

VMEM = pl.BlockSpec(memory_space=pltpu.VMEM)
HBM = pl.BlockSpec(memory_space=pltpu.HBM)
SMEM = pl.BlockSpec(memory_space=pltpu.SMEM)
PARAMS = pltpu.CompilerParams(vmem_limit_bytes=VMEM_LIMIT)
COVER = pl.CostEstimate(flops=int(8e9), bytes_accessed=int(40e6), transcendentals=0)
F32 = jnp.float32
BF16 = jnp.bfloat16


def power(damping_ref, step):
    damping = damping_ref[...]
    coef = damping
    for _ in range(step - 1):
        coef = coef * damping
    return coef


def multiply_tiles(slot_ref, place_ref, count, tile_ref, x_parts, acc_ref, x_ref):
    each = x_ref.shape[0] // len(x_parts)
    for part, part_ref in enumerate(x_parts):
        x_ref[part * each : (part + 1) * each] = part_ref[...]
    acc_ref[...] = jnp.zeros(acc_ref.shape, F32)

    def group(base):
        prods = []
        for lane in range(UNROLL):
            prods.append(
                jnp.dot(x_ref[place_ref[base + lane]], tile_ref[base + lane], preferred_element_type=F32)
            )
        for lane in range(UNROLL):
            slot = slot_ref[base + lane]
            acc_ref[slot] = acc_ref[slot] + prods[lane]

    def chunk_step(chunk, carry):
        for part in range(CHUNK // UNROLL):
            group(chunk * CHUNK + part * UNROLL)
        return carry

    lax.fori_loop(0, (count + CHUNK - 1) // CHUNK, chunk_step, 0)


def first_products(round_index, rows, cols, query_ids, count, col, tiles, n_col, n_row):
    slots, tile, _ = tiles.shape
    queries = query_ids.shape[0]
    col_blocks = n_row * BPD
    row_blocks = n_col * BPD
    spare = n_col * TOUCH
    sent_rows = TOUCH * PLACES
    tile_bits, col_bits, block_bits = (n.bit_length() - 1 for n in (tile, n_col, BPD))

    def body(info_ref, row_ref, col_ref, query_ref, tiles_ref, out_ref, *scratch):
        acc_ref, x_ref, tile_ref, id_rows_ref, asked_ref, has_ref, list_ref, mark_ref, slot_ref, id_ref, sems = scratch
        live, mine, first = info_ref[0], info_ref[1], info_ref[2] * PLACES

        def repeat(times, step, start=0, unroll=8):
            return lax.fori_loop(0, times, step, start, unroll=unroll)

        def clear(ref, value):
            def step(index, carry):
                ref[index] = value
                return carry

            repeat(ref.shape[0], step)

        def copy(index, lane):
            return pltpu.make_async_copy(tiles_ref.at[index], tile_ref.at[lane], sems.at[lane])

        def ask(query, found):
            node = query_ref[query]
            asked_ref[found] = node
            home = (node >> (tile_bits + block_bits)) & (n_col - 1)
            return found + (home == mine).astype(jnp.int32)

        asked = repeat(queries, ask)
        clear(has_ref, 0)
        x_ref[...] = jnp.zeros(x_ref.shape, BF16)
        place_of = lax.broadcasted_iota(jnp.int32, (PLACES, tile), 0)
        node_of = lax.broadcasted_iota(jnp.int32, (PLACES, tile), 1)

        def mark_query(place, carry):
            node = asked_ref[first + place]
            block = (node >> (tile_bits + block_bits + col_bits)) * BPD + ((node >> tile_bits) & (BPD - 1))
            here = (place_of == place) & (node_of == (node & (tile - 1)))
            x_ref[block] = jnp.where(here, 1.0, x_ref[block].astype(F32)).astype(BF16)
            has_ref[block] = 1
            return carry

        lax.fori_loop(0, jnp.clip(asked - first, 0, PLACES), mark_query, 0)

        def pick(index, found):
            list_ref[found] = index
            return found + jnp.where(index < live, has_ref[col_ref[index]], 0)

        found = repeat(slots, pick)

        def start(lane, carry):
            copy(list_ref[lane], lane).start()
            return carry

        lax.fori_loop(0, found, start, 0)
        clear(mark_ref, 0)

        def mark_row(index, carry):
            mark_ref[jnp.where(index < live, row_ref[index], row_blocks)] = 1
            return carry

        repeat(slots, mark_row)
        clear(id_ref, BPD)
        id_rows_ref[...] = jnp.full(id_rows_ref.shape, float(BPD), F32)

        def number_owner(owner, carry):
            rank = 0
            for block in range(BPD):
                marked = mark_ref[owner * BPD + block]
                slot_ref[owner * BPD + block] = owner * TOUCH + rank
                id_ref[owner * TOUCH + rank] = jnp.where(marked > 0, block, BPD)
                rank = rank + marked
            for place in range(TOUCH):
                number = id_ref[owner * TOUCH + place].astype(F32)
                id_rows_ref[owner, place : place + 1] = jnp.full((1, tile), number, F32)
            return carry

        repeat(n_col, number_owner, unroll=1)
        acc_ref[...] = jnp.zeros(acc_ref.shape, F32)

        def step(index, carry):
            prods, goes = [], []
            for lane in range(FIRST_UNROLL):
                at = index * FIRST_UNROLL + lane
                valid = at < found
                which = jnp.where(valid, list_ref[at], 0)

                @pl.when(valid)
                def _():
                    copy(which, at).wait()

                goes.append((at, which, valid))
            for at, which, valid in goes:
                prods.append(
                    lax.dot_general(
                        x_ref[col_ref[which]], tile_ref[at], (((1,), (1,)), ((), ())), preferred_element_type=F32
                    )
                )
            for (at, which, valid), prod in zip(goes, prods):
                slot = jnp.where(valid, slot_ref[row_ref[which]], spare)
                acc_ref[slot] = acc_ref[slot] + prod
            return carry

        lax.fori_loop(0, (found + FIRST_UNROLL - 1) // FIRST_UNROLL, step, 0)
        out_ref[:, :sent_rows] = acc_ref[:spare].astype(BF16).reshape(n_col, sent_rows, tile)
        out_ref[:, sent_rows:] = id_rows_ref[...].astype(BF16)

    info = jnp.stack([count, col, round_index]).astype(jnp.int32)
    return pl.pallas_call(
        body,
        out_shape=jax.ShapeDtypeStruct((n_col, sent_rows + ID_ROWS, tile), BF16),
        in_specs=[SMEM, SMEM, SMEM, SMEM, HBM],
        out_specs=VMEM,
        scratch_shapes=[
            pltpu.VMEM((spare + 1, PLACES, tile), F32),
            pltpu.VMEM((col_blocks, PLACES, tile), BF16),
            pltpu.VMEM(tiles.shape, tiles.dtype),
            pltpu.VMEM((n_col, ID_ROWS, tile), F32),
            pltpu.SMEM((queries,), jnp.int32),
            pltpu.SMEM((col_blocks,), jnp.int32),
            pltpu.SMEM((slots,), jnp.int32),
            pltpu.SMEM((row_blocks + 8,), jnp.int32),
            pltpu.SMEM((row_blocks,), jnp.int32),
            pltpu.SMEM((spare + 8,), jnp.int32),
            pltpu.SemaphoreType.DMA((slots,)),
        ],
        compiler_params=PARAMS,
        name="first_products",
    )(info, rows, cols, query_ids, pltpu.with_memory_space_constraint(tiles, pltpu.HBM))


def products(step, slots, places, count, turned, xparts, owners, damping, owned, scores):
    parts = len(xparts)
    each, width, tile = xparts[0].shape
    rows = TOUCH * width
    before = [] if step == 1 else [scores]

    def body(slot_ref, place_ref, count_ref, tiles_ref, *refs):
        x_refs, (damping_ref, owned_ref), refs = refs[:parts], refs[parts : parts + 2], refs[parts + 2 :]
        score_in, refs = refs[: len(before)], refs[len(before) :]
        out_ref, score_out, score_ref, score_sems, acc_ref, *scratch = refs
        for ref in score_in:
            pltpu.make_async_copy(ref, score_ref, score_sems.at[0]).start()
        multiply_tiles(slot_ref, place_ref, count_ref[0], tiles_ref, x_refs, acc_ref, *scratch)
        for ref in score_in:
            pltpu.make_async_copy(ref, score_ref, score_sems.at[0]).wait()
        if score_in:
            score_ref[...] = score_ref[...] + power(damping_ref, step - 1)[None] * owned_ref[...]
        else:
            score_ref[...] = owned_ref[...]
        leave = pltpu.make_async_copy(score_ref, score_out, score_sems.at[1])
        leave.start()
        out_ref[...] = acc_ref[: owners * TOUCH].astype(BF16).reshape(owners, rows, tile)
        leave.wait()

    return pl.pallas_call(
        body,
        out_shape=(
            jax.ShapeDtypeStruct((owners, rows, tile), BF16),
            pltpu.HBM((BPD, width, tile), F32),
        ),
        in_specs=[SMEM, SMEM, SMEM, VMEM] + [VMEM] * (parts + 2) + [HBM] * len(before),
        out_specs=(VMEM, HBM),
        scratch_shapes=[
            pltpu.VMEM((BPD, width, tile), F32),
            pltpu.SemaphoreType.DMA((2,)),
            pltpu.VMEM((owners * TOUCH + 1, width, tile), F32),
            pltpu.VMEM((parts * each, width, tile), BF16),
        ],
        compiler_params=PARAMS,
        name="products",
    )(
        slots,
        places,
        count,
        turned,
        *xparts,
        damping,
        owned,
        *[pltpu.with_memory_space_constraint(part, pltpu.HBM) for part in before],
    )


def turned_tiles(count, tiles):
    def body(count_ref, tiles_ref, out_ref):
        def group(index, carry):
            for lane in range(UNROLL):
                out_ref[index * UNROLL + lane] = jnp.transpose(tiles_ref[index * UNROLL + lane])
            return carry

        lax.fori_loop(0, (count_ref[0] + UNROLL - 1) // UNROLL, group, 0)

    return pl.pallas_call(
        body,
        out_shape=jax.ShapeDtypeStruct(tiles.shape, tiles.dtype),
        in_specs=[SMEM, VMEM],
        out_specs=VMEM,
        compiler_params=PARAMS,
        name="turned",
    )(count, tiles)


def summed(id_ref, got_ref, acc_ref):
    width = acc_ref.shape[1]
    acc_ref[...] = jnp.zeros(acc_ref.shape, F32)
    for source in range(got_ref.shape[0]):
        for place in range(TOUCH):
            block = id_ref[source * TOUCH + place]
            part = got_ref[source, place * width : (place + 1) * width].astype(F32)
            acc_ref[block] = acc_ref[block] + part


def owned_sum(ids, got, damping):
    width, tile = damping.shape

    def body(id_ref, got_ref, x_ref, out_ref, acc_ref):
        summed(id_ref, got_ref, acc_ref)
        owned = acc_ref[:BPD]
        x_ref[...] = owned.astype(BF16)
        out_ref[...] = owned

    return pl.pallas_call(
        body,
        out_shape=(
            jax.ShapeDtypeStruct((BPD, width, tile), BF16),
            jax.ShapeDtypeStruct((BPD, width, tile), F32),
        ),
        in_specs=[SMEM, VMEM],
        out_specs=(VMEM, VMEM),
        scratch_shapes=[pltpu.VMEM((BPD + 1, width, tile), F32)],
        compiler_params=PARAMS,
        cost_estimate=COVER,
        name="owned",
    )(ids, got)


def placed_sum(ids, got, spread, width, before=()):
    sources, _, tile = got.shape
    queries, columns = spread.shape
    streams = queries // width

    def body(id_ref, got_ref, spread_ref, *refs):
        whole_refs, out_refs, piece_ref = refs[: len(before)], refs[len(before) : -1], refs[-1]
        piece_ref[...] = jnp.zeros(piece_ref.shape, BF16)
        for source in range(sources):
            for place in range(TOUCH):
                block = id_ref[source * TOUCH + place]
                piece_ref[block, source * PLACES : (source + 1) * PLACES] = got_ref[
                    source, place * PLACES : (place + 1) * PLACES
                ]
        for block in range(BPD):
            owned = jnp.dot(spread_ref[...], piece_ref[block], preferred_element_type=F32)
            for stream in range(streams):
                mine = owned[stream * width : (stream + 1) * width]
                if whole_refs:
                    mine = mine + whole_refs[stream][block]
                out_refs[stream][block] = mine

    shape = (BPD, width, tile)
    return pl.pallas_call(
        body,
        out_shape=[jax.ShapeDtypeStruct(shape, F32)] * streams,
        in_specs=[SMEM] + [VMEM] * (2 + len(before)),
        out_specs=[VMEM] * streams,
        scratch_shapes=[pltpu.VMEM((BPD + 1, columns, tile), BF16)],
        compiler_params=PARAMS,
        name="placed",
    )(ids, got, spread, *before)


def rounded(wholes):
    def body(*refs):
        for whole_ref, out_ref in zip(refs[: len(wholes)], refs[len(wholes) :]):
            out_ref[...] = whole_ref[...].astype(BF16)

    return pl.pallas_call(
        body,
        out_shape=[jax.ShapeDtypeStruct(whole.shape, BF16) for whole in wholes],
        in_specs=[VMEM] * len(wholes),
        out_specs=[VMEM] * len(wholes),
        compiler_params=PARAMS,
        cost_estimate=COVER,
        name="rounded",
    )(*wholes)


def ended_sum(step, ids, got, damping, scores):
    width, tile = damping.shape

    def body(id_ref, got_ref, damping_ref, score_ref, out_ref, acc_ref):
        summed(id_ref, got_ref, acc_ref)
        out_ref[...] = score_ref[...] + power(damping_ref, step)[None] * acc_ref[:BPD]

    return pl.pallas_call(
        body,
        out_shape=jax.ShapeDtypeStruct((BPD, width, tile), F32),
        in_specs=[SMEM] + [VMEM] * 3,
        out_specs=VMEM,
        scratch_shapes=[pltpu.VMEM((BPD + 1, width, tile), F32)],
        compiler_params=PARAMS,
        name="ended",
    )(ids, got, damping, scores)


def last_sum(step, ids, got, damping, scores, *done):
    width, tile = damping.shape
    queries = sum(part.shape[1] for part in done) + width

    def body(id_ref, got_ref, damping_ref, score_ref, *refs):
        done_refs, (out_ref, acc_ref) = refs[:-2], refs[-2:]
        summed(id_ref, got_ref, acc_ref)
        coef = power(damping_ref, step)
        for block in range(BPD):
            mine = score_ref[block] + coef * acc_ref[block]
            rows = [part[block] for part in done_refs] + [mine]
            out_ref[block] = jnp.transpose(jnp.concatenate(rows, axis=0))

    return pl.pallas_call(
        body,
        out_shape=jax.ShapeDtypeStruct((BPD, tile, queries), F32),
        in_specs=[SMEM] + [VMEM] * (3 + len(done)),
        out_specs=VMEM,
        scratch_shapes=[pltpu.VMEM((BPD + 1, width, tile), F32)],
        compiler_params=PARAMS,
        name="last",
    )(ids, got, damping, scores, *done)


def row_shift(dz, dcore):
    return [
        (z * N_CORE + core, (z + dz) % N_Z * N_CORE + (core + dcore) % N_CORE)
        for z in range(N_Z)
        for core in range(N_CORE)
    ]


def column_parts(mine):
    same = [mine] + [lax.ppermute(mine, "row", row_shift(dz, 0)) for dz in range(1, N_Z)]
    other = [lax.ppermute(part, "row", row_shift(0, 1)) for part in same]
    return same + other


def after(value, *others):
    return lax.optimization_barrier((value, *others))[0]


def exchange(sent):
    return lax.all_to_all(sent, "col", split_axis=0, concat_axis=0, tiled=True)


def routes(rows, cols, count, n_col):
    slots = rows.shape[0]
    live = jnp.arange(slots, dtype=jnp.int32) < count
    blocks = jnp.arange(n_col * BPD, dtype=jnp.int32)
    hits = (rows[None, :] == blocks[:, None]) & live[None, :]
    marked = jnp.any(hits, axis=1).astype(jnp.int32).reshape(n_col, BPD)
    local = jnp.arange(BPD, dtype=jnp.int32)
    rank = jnp.sum(marked[:, None, :] * (local[None, None, :] < local[None, :, None]), axis=2)
    slot_of = (jnp.arange(n_col, dtype=jnp.int32)[:, None] * TOUCH + rank).reshape(-1)
    slot = jnp.sum(jnp.where(hits, slot_of[:, None], 0), axis=0)
    slot = jnp.where(live, slot, n_col * TOUCH)
    row = lax.axis_index("row")
    owner, block = cols // BPD, cols % BPD
    far = (row // N_CORE - owner // N_CORE) % N_Z
    place = ((row % N_CORE != owner % N_CORE).astype(jnp.int32) * N_Z + far) * BPD + block
    return slot, place


def shards(tiles, tile_row, tile_col, tile_count, query_ids, damping):
    tiles, rows, cols, count = tiles[0, 0], tile_row[0, 0], tile_col[0, 0], tile_count[0, 0]
    tile = tiles.shape[1]
    queries = query_ids.shape[0]
    width = queries // STREAMS
    n_row, n_col = lax.axis_size("row"), lax.axis_size("col")
    col = lax.axis_index("col")

    def first_sent(round_index):
        return first_products(round_index, rows, cols, query_ids, count, col, tiles, n_col, n_row)

    sent = first_sent(0)
    got = exchange(sent)

    later_ids = after(query_ids, sent)
    home = later_ids // (BPD * tile) % n_col
    number = jnp.arange(queries, dtype=jnp.int32)
    same_home = home[:, None] == home[None, :]
    rank = jnp.sum((same_home & (number[None, :] < number[:, None])).astype(jnp.int32), axis=1)
    rounds = jnp.max(rank) // PLACES + 1

    def spread(round_index):
        place = rank - round_index * PLACES
        column = jnp.where((place >= 0) & (place < PLACES), home * PLACES + place, -1)
        return (column[:, None] == jnp.arange(n_col * PLACES, dtype=jnp.int32)[None, :]).astype(BF16)

    slot, place = routes(after(rows, sent), cols, count, n_col)
    turned = turned_tiles(count.reshape(1), after(tiles, sent))
    first_spread = spread(0)
    got_ids = got[:, -ID_ROWS:, 0][:, :TOUCH].astype(jnp.int32).reshape(-1)
    sums = placed_sum(got_ids, after(got, turned, slot, place, first_spread), first_spread, width)

    def next_round(state):
        index, *sums = state
        got = exchange(first_sent(index))
        return index + 1, *placed_sum(got_ids, got, spread(index), width, sums)

    _, *sums = lax.while_loop(lambda state: state[0] < rounds, next_round, (jnp.int32(1), *sums))
    count = count.reshape(1)
    dampings = [
        jnp.broadcast_to(damping[stream * width : (stream + 1) * width][:, None], (width, tile))
        for stream in range(STREAMS)
    ]
    xparts = [column_parts(mine) for mine in rounded(sums)]
    owned, scores = sums, [None] * STREAMS
    for step in range(1, TERMS):
        for stream in range(STREAMS):
            sent, scores[stream] = products(
                step,
                slot,
                place,
                count,
                turned,
                xparts[stream],
                n_col,
                dampings[stream],
                owned[stream],
                scores[stream],
            )
            got = exchange(sent)
            if step + 1 < TERMS:
                mine, owned[stream] = owned_sum(got_ids, got, dampings[stream])
                xparts[stream] = column_parts(mine)
            elif stream + 1 < STREAMS:
                scores[stream] = ended_sum(step, got_ids, got, dampings[stream], scores[stream])
            else:
                total = last_sum(step, got_ids, got, dampings[stream], scores[stream], *scores[:-1])
    return total.reshape(BPD * tile, -1)


def solution(mesh):
    in_specs = (
        P("row", "col", None, None, None),
        P("row", "col", None),
        P("row", "col", None),
        P("row", "col"),
        P(),
        P(),
    )
    out_specs = P(("row", "col"), None)
    return jax.shard_map(shards, mesh=mesh, in_specs=in_specs, out_specs=out_specs, check_vma=False)
```

```python
import jax
import jax.numpy as jnp
from jax import lax
from jax.experimental import pallas as pl
from jax.experimental.pallas import tpu as pltpu
from jax.sharding import PartitionSpec as P


BPD = 8
TERMS = 4
TOUCH = 4
N_Z = 4
N_CORE = 2
STREAMS = 2
PLACES = 32
ID_ROWS = 16
UNROLL = 8
FIRST_UNROLL = 4
CHUNK = 32
VMEM_LIMIT = 14 * 1024 * 1024

VMEM = pl.BlockSpec(memory_space=pltpu.VMEM)
HBM = pl.BlockSpec(memory_space=pltpu.HBM)
SMEM = pl.BlockSpec(memory_space=pltpu.SMEM)
PARAMS = pltpu.CompilerParams(vmem_limit_bytes=VMEM_LIMIT)
COVER = pl.CostEstimate(flops=int(8e9), bytes_accessed=int(40e6), transcendentals=0)
F32 = jnp.float32
BF16 = jnp.bfloat16


def power(damping_ref, step):
    damping = damping_ref[...]
    coef = damping
    for _ in range(step - 1):
        coef = coef * damping
    return coef


def multiply_tiles(slot_ref, place_ref, count, tile_ref, x_parts, acc_ref, x_ref):
    each = x_ref.shape[0] // len(x_parts)
    for part, part_ref in enumerate(x_parts):
        x_ref[part * each : (part + 1) * each] = part_ref[...]
    acc_ref[...] = jnp.zeros(acc_ref.shape, F32)

    def group(base):
        prods = []
        for lane in range(UNROLL):
            prods.append(
                jnp.dot(x_ref[place_ref[base + lane]], tile_ref[base + lane], preferred_element_type=F32)
            )
        for lane in range(UNROLL):
            slot = slot_ref[base + lane]
            acc_ref[slot] = acc_ref[slot] + prods[lane]

    def chunk_step(chunk, carry):
        for part in range(CHUNK // UNROLL):
            group(chunk * CHUNK + part * UNROLL)
        return carry

    lax.fori_loop(0, (count + CHUNK - 1) // CHUNK, chunk_step, 0)


def first_products(round_index, rows, cols, query_ids, count, col, tiles, n_col, n_row):
    slots, tile, _ = tiles.shape
    queries = query_ids.shape[0]
    col_blocks = n_row * BPD
    row_blocks = n_col * BPD
    spare = n_col * TOUCH
    sent_rows = TOUCH * PLACES
    tile_bits, col_bits, block_bits = (n.bit_length() - 1 for n in (tile, n_col, BPD))

    def body(info_ref, row_ref, col_ref, query_ref, tiles_ref, out_ref, *scratch):
        acc_ref, x_ref, tile_ref, id_rows_ref, asked_ref, has_ref, list_ref, mark_ref, slot_ref, id_ref, sems = scratch
        live, mine, first = info_ref[0], info_ref[1], info_ref[2] * PLACES

        def repeat(times, step, start=0, unroll=8):
            return lax.fori_loop(0, times, step, start, unroll=unroll)

        def clear(ref, value):
            def step(index, carry):
                ref[index] = value
                return carry

            repeat(ref.shape[0], step)

        def copy(index, lane):
            return pltpu.make_async_copy(tiles_ref.at[index], tile_ref.at[lane], sems.at[lane])

        def ask(query, found):
            node = query_ref[query]
            asked_ref[found] = node
            home = (node >> (tile_bits + block_bits)) & (n_col - 1)
            return found + (home == mine).astype(jnp.int32)

        asked = repeat(queries, ask)
        clear(has_ref, 0)
        x_ref[...] = jnp.zeros(x_ref.shape, BF16)
        place_of = lax.broadcasted_iota(jnp.int32, (PLACES, tile), 0)
        node_of = lax.broadcasted_iota(jnp.int32, (PLACES, tile), 1)

        def mark_query(place, carry):
            node = asked_ref[first + place]
            block = (node >> (tile_bits + block_bits + col_bits)) * BPD + ((node >> tile_bits) & (BPD - 1))
            here = (place_of == place) & (node_of == (node & (tile - 1)))
            x_ref[block] = jnp.where(here, 1.0, x_ref[block].astype(F32)).astype(BF16)
            has_ref[block] = 1
            return carry

        lax.fori_loop(0, jnp.clip(asked - first, 0, PLACES), mark_query, 0)

        def pick(index, found):
            list_ref[found] = index
            return found + jnp.where(index < live, has_ref[col_ref[index]], 0)

        found = repeat(slots, pick)

        def start(lane, carry):
            copy(list_ref[lane], lane).start()
            return carry

        lax.fori_loop(0, found, start, 0)
        clear(mark_ref, 0)

        def mark_row(index, carry):
            mark_ref[jnp.where(index < live, row_ref[index], row_blocks)] = 1
            return carry

        repeat(slots, mark_row)
        clear(id_ref, BPD)
        id_rows_ref[...] = jnp.full(id_rows_ref.shape, float(BPD), F32)

        def number_owner(owner, carry):
            rank = 0
            for block in range(BPD):
                marked = mark_ref[owner * BPD + block]
                slot_ref[owner * BPD + block] = owner * TOUCH + rank
                id_ref[owner * TOUCH + rank] = jnp.where(marked > 0, block, BPD)
                rank = rank + marked
            for place in range(TOUCH):
                number = id_ref[owner * TOUCH + place].astype(F32)
                id_rows_ref[owner, place : place + 1] = jnp.full((1, tile), number, F32)
            return carry

        repeat(n_col, number_owner, unroll=1)
        acc_ref[...] = jnp.zeros(acc_ref.shape, F32)

        def step(index, carry):
            prods, goes = [], []
            for lane in range(FIRST_UNROLL):
                at = index * FIRST_UNROLL + lane
                valid = at < found
                which = jnp.where(valid, list_ref[at], 0)

                @pl.when(valid)
                def _():
                    copy(which, at).wait()

                goes.append((at, which, valid))
            for at, which, valid in goes:
                prods.append(
                    lax.dot_general(
                        x_ref[col_ref[which]], tile_ref[at], (((1,), (1,)), ((), ())), preferred_element_type=F32
                    )
                )
            for (at, which, valid), prod in zip(goes, prods):
                slot = jnp.where(valid, slot_ref[row_ref[which]], spare)
                acc_ref[slot] = acc_ref[slot] + prod
            return carry

        lax.fori_loop(0, (found + FIRST_UNROLL - 1) // FIRST_UNROLL, step, 0)
        out_ref[:, :sent_rows] = acc_ref[:spare].astype(BF16).reshape(n_col, sent_rows, tile)
        out_ref[:, sent_rows:] = id_rows_ref[...].astype(BF16)

    info = jnp.stack([count, col, round_index]).astype(jnp.int32)
    return pl.pallas_call(
        body,
        out_shape=jax.ShapeDtypeStruct((n_col, sent_rows + ID_ROWS, tile), BF16),
        in_specs=[SMEM, SMEM, SMEM, SMEM, HBM],
        out_specs=VMEM,
        scratch_shapes=[
            pltpu.VMEM((spare + 1, PLACES, tile), F32),
            pltpu.VMEM((col_blocks, PLACES, tile), BF16),
            pltpu.VMEM(tiles.shape, tiles.dtype),
            pltpu.VMEM((n_col, ID_ROWS, tile), F32),
            pltpu.SMEM((queries,), jnp.int32),
            pltpu.SMEM((col_blocks,), jnp.int32),
            pltpu.SMEM((slots,), jnp.int32),
            pltpu.SMEM((row_blocks + 8,), jnp.int32),
            pltpu.SMEM((row_blocks,), jnp.int32),
            pltpu.SMEM((spare + 8,), jnp.int32),
            pltpu.SemaphoreType.DMA((slots,)),
        ],
        compiler_params=PARAMS,
        name="first_products",
    )(info, rows, cols, query_ids, pltpu.with_memory_space_constraint(tiles, pltpu.HBM))


def products(step, slots, places, count, turned, xparts, owners, damping, owned, scores):
    parts = len(xparts)
    each, width, tile = xparts[0].shape
    rows = TOUCH * width
    before = [] if step == 1 else [scores]

    def body(slot_ref, place_ref, count_ref, tiles_ref, *refs):
        x_refs, (damping_ref, owned_ref), refs = refs[:parts], refs[parts : parts + 2], refs[parts + 2 :]
        score_in, refs = refs[: len(before)], refs[len(before) :]
        out_ref, score_out, score_ref, score_sems, acc_ref, *scratch = refs
        for ref in score_in:
            pltpu.make_async_copy(ref, score_ref, score_sems.at[0]).start()
        multiply_tiles(slot_ref, place_ref, count_ref[0], tiles_ref, x_refs, acc_ref, *scratch)
        for ref in score_in:
            pltpu.make_async_copy(ref, score_ref, score_sems.at[0]).wait()
        if score_in:
            score_ref[...] = score_ref[...] + power(damping_ref, step - 1)[None] * owned_ref[...]
        else:
            score_ref[...] = owned_ref[...]
        leave = pltpu.make_async_copy(score_ref, score_out, score_sems.at[1])
        leave.start()
        out_ref[...] = acc_ref[: owners * TOUCH].astype(BF16).reshape(owners, rows, tile)
        leave.wait()

    return pl.pallas_call(
        body,
        out_shape=(
            jax.ShapeDtypeStruct((owners, rows, tile), BF16),
            pltpu.HBM((BPD, width, tile), F32),
        ),
        in_specs=[SMEM, SMEM, SMEM, VMEM] + [VMEM] * (parts + 2) + [HBM] * len(before),
        out_specs=(VMEM, HBM),
        scratch_shapes=[
            pltpu.VMEM((BPD, width, tile), F32),
            pltpu.SemaphoreType.DMA((2,)),
            pltpu.VMEM((owners * TOUCH + 1, width, tile), F32),
            pltpu.VMEM((parts * each, width, tile), BF16),
        ],
        compiler_params=PARAMS,
        name="products",
    )(
        slots,
        places,
        count,
        turned,
        *xparts,
        damping,
        owned,
        *[pltpu.with_memory_space_constraint(part, pltpu.HBM) for part in before],
    )


def turned_tiles(count, tiles):
    def body(count_ref, tiles_ref, out_ref):
        def group(index, carry):
            for lane in range(UNROLL):
                out_ref[index * UNROLL + lane] = jnp.transpose(tiles_ref[index * UNROLL + lane])
            return carry

        lax.fori_loop(0, (count_ref[0] + UNROLL - 1) // UNROLL, group, 0)

    return pl.pallas_call(
        body,
        out_shape=jax.ShapeDtypeStruct(tiles.shape, tiles.dtype),
        in_specs=[SMEM, VMEM],
        out_specs=VMEM,
        compiler_params=PARAMS,
        name="turned",
    )(count, tiles)


def summed(id_ref, got_ref, acc_ref):
    width = acc_ref.shape[1]
    acc_ref[...] = jnp.zeros(acc_ref.shape, F32)
    for source in range(got_ref.shape[0]):
        for place in range(TOUCH):
            block = id_ref[source * TOUCH + place]
            part = got_ref[source, place * width : (place + 1) * width].astype(F32)
            acc_ref[block] = acc_ref[block] + part


def owned_sum(ids, got, damping):
    width, tile = damping.shape

    def body(id_ref, got_ref, x_ref, out_ref, acc_ref):
        summed(id_ref, got_ref, acc_ref)
        owned = acc_ref[:BPD]
        x_ref[...] = owned.astype(BF16)
        out_ref[...] = owned

    return pl.pallas_call(
        body,
        out_shape=(
            jax.ShapeDtypeStruct((BPD, width, tile), BF16),
            jax.ShapeDtypeStruct((BPD, width, tile), F32),
        ),
        in_specs=[SMEM, VMEM],
        out_specs=(VMEM, VMEM),
        scratch_shapes=[pltpu.VMEM((BPD + 1, width, tile), F32)],
        compiler_params=PARAMS,
        cost_estimate=COVER,
        name="owned",
    )(ids, got)


def placed_sum(ids, got, spread, width, before=()):
    sources, _, tile = got.shape
    queries, columns = spread.shape
    streams = queries // width

    def body(id_ref, got_ref, spread_ref, *refs):
        whole_refs, out_refs, piece_ref = refs[: len(before)], refs[len(before) : -1], refs[-1]
        piece_ref[...] = jnp.zeros(piece_ref.shape, BF16)
        for source in range(sources):
            for place in range(TOUCH):
                block = id_ref[source * TOUCH + place]
                piece_ref[block, source * PLACES : (source + 1) * PLACES] = got_ref[
                    source, place * PLACES : (place + 1) * PLACES
                ]
        for block in range(BPD):
            owned = jnp.dot(spread_ref[...], piece_ref[block], preferred_element_type=F32)
            for stream in range(streams):
                mine = owned[stream * width : (stream + 1) * width]
                if whole_refs:
                    mine = mine + whole_refs[stream][block]
                out_refs[stream][block] = mine

    shape = (BPD, width, tile)
    return pl.pallas_call(
        body,
        out_shape=[jax.ShapeDtypeStruct(shape, F32)] * streams,
        in_specs=[SMEM] + [VMEM] * (2 + len(before)),
        out_specs=[VMEM] * streams,
        scratch_shapes=[pltpu.VMEM((BPD + 1, columns, tile), BF16)],
        compiler_params=PARAMS,
        name="placed",
    )(ids, got, spread, *before)


def rounded(whole):
    def body(whole_ref, out_ref):
        out_ref[...] = whole_ref[...].astype(BF16)

    return pl.pallas_call(
        body,
        out_shape=jax.ShapeDtypeStruct(whole.shape, BF16),
        in_specs=[VMEM],
        out_specs=VMEM,
        compiler_params=PARAMS,
        cost_estimate=COVER,
        name="rounded",
    )(whole)


def ended_sum(step, ids, got, damping, scores):
    width, tile = damping.shape

    def body(id_ref, got_ref, damping_ref, score_ref, out_ref, acc_ref):
        summed(id_ref, got_ref, acc_ref)
        out_ref[...] = score_ref[...] + power(damping_ref, step)[None] * acc_ref[:BPD]

    return pl.pallas_call(
        body,
        out_shape=jax.ShapeDtypeStruct((BPD, width, tile), F32),
        in_specs=[SMEM] + [VMEM] * 3,
        out_specs=VMEM,
        scratch_shapes=[pltpu.VMEM((BPD + 1, width, tile), F32)],
        compiler_params=PARAMS,
        name="ended",
    )(ids, got, damping, scores)


def last_sum(step, ids, got, damping, scores, *done):
    width, tile = damping.shape
    queries = sum(part.shape[1] for part in done) + width

    def body(id_ref, got_ref, damping_ref, score_ref, *refs):
        done_refs, (out_ref, acc_ref) = refs[:-2], refs[-2:]
        summed(id_ref, got_ref, acc_ref)
        coef = power(damping_ref, step)
        for block in range(BPD):
            mine = score_ref[block] + coef * acc_ref[block]
            rows = [part[block] for part in done_refs] + [mine]
            out_ref[block] = jnp.transpose(jnp.concatenate(rows, axis=0))

    return pl.pallas_call(
        body,
        out_shape=jax.ShapeDtypeStruct((BPD, tile, queries), F32),
        in_specs=[SMEM] + [VMEM] * (3 + len(done)),
        out_specs=VMEM,
        scratch_shapes=[pltpu.VMEM((BPD + 1, width, tile), F32)],
        compiler_params=PARAMS,
        name="last",
    )(ids, got, damping, scores, *done)


def row_shift(dz, dcore):
    return [
        (z * N_CORE + core, (z + dz) % N_Z * N_CORE + (core + dcore) % N_CORE)
        for z in range(N_Z)
        for core in range(N_CORE)
    ]


def column_parts(mine):
    same = [mine] + [lax.ppermute(mine, "row", row_shift(dz, 0)) for dz in range(1, N_Z)]
    other = [lax.ppermute(part, "row", row_shift(0, 1)) for part in same]
    return same + other


def after(value, *others):
    return lax.optimization_barrier((value, *others))[0]


def exchange(sent):
    return lax.all_to_all(sent, "col", split_axis=0, concat_axis=0, tiled=True)


def routes(rows, cols, count, n_col):
    slots = rows.shape[0]
    live = jnp.arange(slots, dtype=jnp.int32) < count
    blocks = jnp.arange(n_col * BPD, dtype=jnp.int32)
    hits = (rows[None, :] == blocks[:, None]) & live[None, :]
    marked = jnp.any(hits, axis=1).astype(jnp.int32).reshape(n_col, BPD)
    local = jnp.arange(BPD, dtype=jnp.int32)
    rank = jnp.sum(marked[:, None, :] * (local[None, None, :] < local[None, :, None]), axis=2)
    slot_of = (jnp.arange(n_col, dtype=jnp.int32)[:, None] * TOUCH + rank).reshape(-1)
    slot = jnp.sum(jnp.where(hits, slot_of[:, None], 0), axis=0)
    slot = jnp.where(live, slot, n_col * TOUCH)
    row = lax.axis_index("row")
    owner, block = cols // BPD, cols % BPD
    far = (row // N_CORE - owner // N_CORE) % N_Z
    place = ((row % N_CORE != owner % N_CORE).astype(jnp.int32) * N_Z + far) * BPD + block
    return slot, place


def shards(tiles, tile_row, tile_col, tile_count, query_ids, damping):
    tiles, rows, cols, count = tiles[0, 0], tile_row[0, 0], tile_col[0, 0], tile_count[0, 0]
    tile = tiles.shape[1]
    queries = query_ids.shape[0]
    width = queries // STREAMS
    n_row, n_col = lax.axis_size("row"), lax.axis_size("col")
    col = lax.axis_index("col")

    def first_sent(round_index):
        return first_products(round_index, rows, cols, query_ids, count, col, tiles, n_col, n_row)

    sent = first_sent(0)
    got = exchange(sent)

    later_ids = after(query_ids, sent)
    home = later_ids // (BPD * tile) % n_col
    number = jnp.arange(queries, dtype=jnp.int32)
    same_home = home[:, None] == home[None, :]
    rank = jnp.sum((same_home & (number[None, :] < number[:, None])).astype(jnp.int32), axis=1)
    rounds = jnp.max(rank) // PLACES + 1

    def spread(round_index):
        place = rank - round_index * PLACES
        column = jnp.where((place >= 0) & (place < PLACES), home * PLACES + place, -1)
        return (column[:, None] == jnp.arange(n_col * PLACES, dtype=jnp.int32)[None, :]).astype(BF16)

    slot, place = routes(after(rows, sent), cols, count, n_col)
    turned = turned_tiles(count.reshape(1), after(tiles, sent))
    first_spread = spread(0)
    got_ids = got[:, -ID_ROWS:, 0][:, :TOUCH].astype(jnp.int32).reshape(-1)
    sums = placed_sum(got_ids, after(got, turned, slot, place, first_spread), first_spread, width)

    def next_round(state):
        index, *sums = state
        got = exchange(first_sent(index))
        return index + 1, *placed_sum(got_ids, got, spread(index), width, sums)

    _, *sums = lax.while_loop(lambda state: state[0] < rounds, next_round, (jnp.int32(1), *sums))
    count = count.reshape(1)
    dampings = [
        jnp.broadcast_to(damping[stream * width : (stream + 1) * width][:, None], (width, tile))
        for stream in range(STREAMS)
    ]
    xparts = [None] * STREAMS
    owned, scores = sums, [None] * STREAMS
    for step in range(1, TERMS):
        for stream in range(STREAMS):
            if step == 1:
                mine = rounded(after(owned[stream], sent) if stream else owned[stream])
                xparts[stream] = column_parts(mine)
            sent, scores[stream] = products(
                step,
                slot,
                place,
                count,
                turned,
                xparts[stream],
                n_col,
                dampings[stream],
                owned[stream],
                scores[stream],
            )
            got = exchange(sent)
            if step + 1 < TERMS:
                mine, owned[stream] = owned_sum(got_ids, got, dampings[stream])
                xparts[stream] = column_parts(mine)
            elif stream + 1 < STREAMS:
                scores[stream] = ended_sum(step, got_ids, got, dampings[stream], scores[stream])
            else:
                total = last_sum(step, got_ids, got, dampings[stream], scores[stream], *scores[:-1])
    return total.reshape(BPD * tile, -1)


def solution(mesh):
    in_specs = (
        P("row", "col", None, None, None),
        P("row", "col", None),
        P("row", "col", None),
        P("row", "col"),
        P(),
        P(),
    )
    out_specs = P(("row", "col"), None)
    return jax.shard_map(shards, mesh=mesh, in_specs=in_specs, out_specs=out_specs, check_vma=False)
```

```python
import jax
import jax.numpy as jnp
from jax import lax
from jax.experimental import pallas as pl
from jax.experimental.pallas import tpu as pltpu
from jax.sharding import PartitionSpec as P


BPD = 8
TERMS = 4
TOUCH = 4
N_Z = 4
N_CORE = 2
N_X = 4
STREAMS = 2
PLACES = 24
ID_ROWS = 16
UNROLL = 8
FIRST_UNROLL = 8
CHUNK = 32
VMEM_LIMIT = 14 * 1024 * 1024

VMEM = pl.BlockSpec(memory_space=pltpu.VMEM)
HBM = pl.BlockSpec(memory_space=pltpu.HBM)
SMEM = pl.BlockSpec(memory_space=pltpu.SMEM)
PARAMS = pltpu.CompilerParams(vmem_limit_bytes=VMEM_LIMIT)
COVER = pl.CostEstimate(flops=int(8e9), bytes_accessed=int(40e6), transcendentals=0)
F32 = jnp.float32
BF16 = jnp.bfloat16


def power(damping_ref, step):
    damping = damping_ref[...]
    coef = damping
    for _ in range(step - 1):
        coef = coef * damping
    return coef


def multiply_tiles(slot_ref, place_ref, count, tile_ref, x_parts, acc_ref, x_ref):
    each = x_ref.shape[0] // len(x_parts)
    for part, part_ref in enumerate(x_parts):
        x_ref[part * each : (part + 1) * each] = part_ref[...]
    acc_ref[...] = jnp.zeros(acc_ref.shape, F32)

    def group(base):
        prods = []
        for lane in range(UNROLL):
            prods.append(
                jnp.dot(x_ref[place_ref[base + lane]], tile_ref[base + lane], preferred_element_type=F32)
            )
        for lane in range(UNROLL):
            slot = slot_ref[base + lane]
            acc_ref[slot] = acc_ref[slot] + prods[lane]

    def chunk_step(chunk, carry):
        for part in range(CHUNK // UNROLL):
            group(chunk * CHUNK + part * UNROLL)
        return carry

    lax.fori_loop(0, (count + CHUNK - 1) // CHUNK, chunk_step, 0)


def first_products(round_index, rows, cols, query_ids, count, col, tiles, n_col, n_row):
    slots, tile, _ = tiles.shape
    queries = query_ids.shape[0]
    col_blocks = n_row * BPD
    row_blocks = n_col * BPD
    spare = n_col * TOUCH
    sent_rows = TOUCH * PLACES
    tile_bits, col_bits, block_bits = (n.bit_length() - 1 for n in (tile, n_col, BPD))

    def body(info_ref, row_ref, col_ref, query_ref, tiles_ref, out_ref, *scratch):
        acc_ref, x_ref, tile_ref, id_rows_ref, asked_ref, has_ref, list_ref, mark_ref, slot_ref, id_ref, sems = scratch
        live, mine, first = info_ref[0], info_ref[1], info_ref[2] * PLACES

        def repeat(times, step, start=0, unroll=8):
            return lax.fori_loop(0, times, step, start, unroll=unroll)

        def clear(ref, value):
            def step(index, carry):
                ref[index] = value
                return carry

            repeat(ref.shape[0], step)

        def copy(index, lane):
            return pltpu.make_async_copy(tiles_ref.at[index], tile_ref.at[lane], sems.at[lane])

        def ask(query, found):
            node = query_ref[query]
            asked_ref[found] = node
            home = (node >> (tile_bits + block_bits)) & (n_col - 1)
            return found + (home == mine).astype(jnp.int32)

        asked = repeat(queries, ask)
        clear(has_ref, 0)
        x_ref[...] = jnp.zeros(x_ref.shape, BF16)
        place_of = lax.broadcasted_iota(jnp.int32, (PLACES, tile), 0)
        node_of = lax.broadcasted_iota(jnp.int32, (PLACES, tile), 1)

        def mark_query(place, carry):
            node = asked_ref[first + place]
            block = (node >> (tile_bits + block_bits + col_bits)) * BPD + ((node >> tile_bits) & (BPD - 1))
            here = (place_of == place) & (node_of == (node & (tile - 1)))
            x_ref[block] = jnp.where(here, 1.0, x_ref[block].astype(F32)).astype(BF16)
            has_ref[block] = 1
            return carry

        lax.fori_loop(0, jnp.clip(asked - first, 0, PLACES), mark_query, 0)

        def pick(index, found):
            list_ref[found] = index
            return found + jnp.where(index < live, has_ref[col_ref[index]], 0)

        found = repeat(slots, pick)

        def start(lane, carry):
            copy(list_ref[lane], lane).start()
            return carry

        lax.fori_loop(0, found, start, 0)
        clear(mark_ref, 0)

        def mark_row(index, carry):
            mark_ref[jnp.where(index < live, row_ref[index], row_blocks)] = 1
            return carry

        repeat(slots, mark_row)
        clear(id_ref, BPD)
        id_rows_ref[...] = jnp.full(id_rows_ref.shape, float(BPD), F32)

        def number_owner(owner, sent_to):
            rank = 0
            for block in range(BPD):
                marked = mark_ref[owner * BPD + block]
                slot_ref[owner * BPD + block] = sent_to * TOUCH + rank
                id_ref[sent_to * TOUCH + rank] = jnp.where(marked > 0, block, BPD)
                rank = rank + marked
            for place in range(TOUCH):
                number = id_ref[sent_to * TOUCH + place].astype(F32)
                id_rows_ref[sent_to, place : place + 1] = jnp.full((1, tile), number, F32)

        for sent_to, owner in enumerate(exchange_order(n_col)):
            number_owner(owner, sent_to)
        acc_ref[...] = jnp.zeros(acc_ref.shape, F32)

        def step(index, carry):
            prods, goes = [], []
            for lane in range(FIRST_UNROLL):
                at = index * FIRST_UNROLL + lane
                valid = at < found
                which = jnp.where(valid, list_ref[at], 0)

                @pl.when(valid)
                def _():
                    copy(which, at).wait()

                goes.append((at, which, valid))
            for at, which, valid in goes:
                prods.append(
                    lax.dot_general(
                        x_ref[col_ref[which]], tile_ref[at], (((1,), (1,)), ((), ())), preferred_element_type=F32
                    )
                )
            for (at, which, valid), prod in zip(goes, prods):
                slot = jnp.where(valid, slot_ref[row_ref[which]], spare)
                acc_ref[slot] = acc_ref[slot] + prod
            return carry

        lax.fori_loop(0, (found + FIRST_UNROLL - 1) // FIRST_UNROLL, step, 0)
        out_ref[:, :sent_rows] = acc_ref[:spare].reshape(n_col, sent_rows, tile).astype(BF16)
        out_ref[:, sent_rows:] = id_rows_ref[...].astype(BF16)

    info = jnp.stack([count, col, round_index]).astype(jnp.int32)
    return pl.pallas_call(
        body,
        out_shape=jax.ShapeDtypeStruct((n_col, sent_rows + ID_ROWS, tile), BF16),
        in_specs=[SMEM, SMEM, SMEM, SMEM, HBM],
        out_specs=VMEM,
        scratch_shapes=[
            pltpu.VMEM((spare + 1, PLACES, tile), F32),
            pltpu.VMEM((col_blocks, PLACES, tile), BF16),
            pltpu.VMEM(tiles.shape, tiles.dtype),
            pltpu.VMEM((n_col, ID_ROWS, tile), F32),
            pltpu.SMEM((queries,), jnp.int32),
            pltpu.SMEM((col_blocks,), jnp.int32),
            pltpu.SMEM((slots,), jnp.int32),
            pltpu.SMEM((row_blocks + 8,), jnp.int32),
            pltpu.SMEM((row_blocks,), jnp.int32),
            pltpu.SMEM((spare + 8,), jnp.int32),
            pltpu.SemaphoreType.DMA((slots,)),
        ],
        compiler_params=PARAMS,
        name="first_products",
    )(info, rows, cols, query_ids, pltpu.with_memory_space_constraint(tiles, pltpu.HBM))


def products(step, slots, places, count, turned, xparts, owners, damping, owned, scores):
    parts = len(xparts)
    each, width, tile = xparts[0].shape
    rows = TOUCH * width
    before = [] if step == 1 else [scores]

    def body(slot_ref, place_ref, count_ref, tiles_ref, *refs):
        x_refs, (damping_ref, owned_ref), refs = refs[:parts], refs[parts : parts + 2], refs[parts + 2 :]
        score_in, refs = refs[: len(before)], refs[len(before) :]
        out_ref, score_out, score_ref, score_sems, acc_ref, *scratch = refs
        for ref in score_in:
            pltpu.make_async_copy(ref, score_ref, score_sems.at[0]).start()
        multiply_tiles(slot_ref, place_ref, count_ref[0], tiles_ref, x_refs, acc_ref, *scratch)
        for ref in score_in:
            pltpu.make_async_copy(ref, score_ref, score_sems.at[0]).wait()
        if score_in:
            score_ref[...] = score_ref[...] + power(damping_ref, step - 1)[None] * owned_ref[...]
        else:
            score_ref[...] = owned_ref[...]
        leave = pltpu.make_async_copy(score_ref, score_out, score_sems.at[1])
        leave.start()
        out_ref[...] = acc_ref[: owners * TOUCH].astype(BF16).reshape(owners, rows, tile)
        leave.wait()

    return pl.pallas_call(
        body,
        out_shape=(
            jax.ShapeDtypeStruct((owners, rows, tile), BF16),
            pltpu.HBM((BPD, width, tile), F32),
        ),
        in_specs=[SMEM, SMEM, SMEM, VMEM] + [VMEM] * (parts + 2) + [HBM] * len(before),
        out_specs=(VMEM, HBM),
        scratch_shapes=[
            pltpu.VMEM((BPD, width, tile), F32),
            pltpu.SemaphoreType.DMA((2,)),
            pltpu.VMEM((owners * TOUCH + 1, width, tile), F32),
            pltpu.VMEM((parts * each, width, tile), BF16),
        ],
        compiler_params=PARAMS,
        name="products",
    )(
        slots,
        places,
        count,
        turned,
        *xparts,
        damping,
        owned,
        *[pltpu.with_memory_space_constraint(part, pltpu.HBM) for part in before],
    )


def turned_tiles(count, tiles):
    def body(count_ref, tiles_ref, out_ref):
        def group(index, carry):
            for lane in range(UNROLL):
                out_ref[index * UNROLL + lane] = jnp.transpose(tiles_ref[index * UNROLL + lane])
            return carry

        lax.fori_loop(0, (count_ref[0] + UNROLL - 1) // UNROLL, group, 0)

    return pl.pallas_call(
        body,
        out_shape=jax.ShapeDtypeStruct(tiles.shape, tiles.dtype),
        in_specs=[SMEM, VMEM],
        out_specs=VMEM,
        compiler_params=PARAMS,
        name="turned",
    )(count, tiles)


def summed(id_ref, got_ref, acc_ref):
    width = acc_ref.shape[1]
    acc_ref[...] = jnp.zeros(acc_ref.shape, F32)
    for source in range(got_ref.shape[0]):
        for place in range(TOUCH):
            block = id_ref[source * TOUCH + place]
            part = got_ref[source, place * width : (place + 1) * width].astype(F32)
            acc_ref[block] = acc_ref[block] + part


def owned_sum(ids, got, damping):
    width, tile = damping.shape

    def body(id_ref, got_ref, x_ref, out_ref, acc_ref):
        summed(id_ref, got_ref, acc_ref)
        owned = acc_ref[:BPD]
        x_ref[...] = owned.astype(BF16)
        out_ref[...] = owned

    return pl.pallas_call(
        body,
        out_shape=(
            jax.ShapeDtypeStruct((BPD, width, tile), BF16),
            jax.ShapeDtypeStruct((BPD, width, tile), F32),
        ),
        in_specs=[SMEM, VMEM],
        out_specs=(VMEM, VMEM),
        scratch_shapes=[pltpu.VMEM((BPD + 1, width, tile), F32)],
        compiler_params=PARAMS,
        cost_estimate=COVER,
        name="owned",
    )(ids, got)


def placed_sum(ids, got, spread, width, before=()):
    sources, _, tile = got.shape
    queries, columns = spread.shape
    streams = queries // width

    def body(id_ref, got_ref, spread_ref, *refs):
        whole_refs, out_refs, piece_ref = refs[: len(before)], refs[len(before) : -1], refs[-1]
        piece_ref[...] = jnp.zeros(piece_ref.shape, F32)
        for source in range(sources):
            part = got_ref[source].astype(F32)
            for place in range(TOUCH):
                block = id_ref[source * TOUCH + place]
                piece_ref[block, source * PLACES : (source + 1) * PLACES] = part[
                    place * PLACES : (place + 1) * PLACES
                ]
        for block in range(BPD):
            owned = jnp.dot(spread_ref[...], piece_ref[block].astype(BF16), preferred_element_type=F32)
            for stream in range(streams):
                mine = owned[stream * width : (stream + 1) * width]
                if whole_refs:
                    mine = mine + whole_refs[stream][block]
                out_refs[stream][block] = mine

    shape = (BPD, width, tile)
    return pl.pallas_call(
        body,
        out_shape=[jax.ShapeDtypeStruct(shape, F32)] * streams,
        in_specs=[SMEM] + [VMEM] * (2 + len(before)),
        out_specs=[VMEM] * streams,
        scratch_shapes=[pltpu.VMEM((BPD + 1, columns, tile), F32)],
        compiler_params=PARAMS,
        name="placed",
    )(ids, got, spread, *before)


def rounded(whole):
    def body(whole_ref, out_ref):
        out_ref[...] = whole_ref[...].astype(BF16)

    return pl.pallas_call(
        body,
        out_shape=jax.ShapeDtypeStruct(whole.shape, BF16),
        in_specs=[VMEM],
        out_specs=VMEM,
        compiler_params=PARAMS,
        cost_estimate=COVER,
        name="rounded",
    )(whole)


def ended_sum(step, ids, got, damping, scores):
    width, tile = damping.shape

    def body(id_ref, got_ref, damping_ref, score_ref, out_ref, acc_ref):
        summed(id_ref, got_ref, acc_ref)
        out_ref[...] = score_ref[...] + power(damping_ref, step)[None] * acc_ref[:BPD]

    return pl.pallas_call(
        body,
        out_shape=jax.ShapeDtypeStruct((BPD, width, tile), F32),
        in_specs=[SMEM] + [VMEM] * 3,
        out_specs=VMEM,
        scratch_shapes=[pltpu.VMEM((BPD + 1, width, tile), F32)],
        compiler_params=PARAMS,
        name="ended",
    )(ids, got, damping, scores)


def last_sum(step, ids, got, damping, scores, *done):
    width, tile = damping.shape
    queries = sum(part.shape[1] for part in done) + width

    def body(id_ref, got_ref, damping_ref, score_ref, *refs):
        done_refs, (out_ref, acc_ref) = refs[:-2], refs[-2:]
        summed(id_ref, got_ref, acc_ref)
        coef = power(damping_ref, step)
        for block in range(BPD):
            mine = score_ref[block] + coef * acc_ref[block]
            rows = [part[block] for part in done_refs] + [mine]
            out_ref[block] = jnp.transpose(jnp.concatenate(rows, axis=0))

    return pl.pallas_call(
        body,
        out_shape=jax.ShapeDtypeStruct((BPD, tile, queries), F32),
        in_specs=[SMEM] + [VMEM] * (3 + len(done)),
        out_specs=VMEM,
        scratch_shapes=[pltpu.VMEM((BPD + 1, width, tile), F32)],
        compiler_params=PARAMS,
        name="last",
    )(ids, got, damping, scores, *done)


def row_shift(dz, dcore):
    return [
        (z * N_CORE + core, (z + dz) % N_Z * N_CORE + (core + dcore) % N_CORE)
        for z in range(N_Z)
        for core in range(N_CORE)
    ]


def column_parts(mine):
    same = [mine] + [lax.ppermute(mine, "row", row_shift(dz, 0)) for dz in range(1, N_Z)]
    other = [lax.ppermute(part, "row", row_shift(0, 1)) for part in same]
    return same + other


def after(value, *others):
    return lax.optimization_barrier((value, *others))[0]


def exchange_order(n_col):
    n_y = n_col // N_X
    return [x * n_y + (y if x % 2 == 0 else n_y - 1 - y) for x in range(N_X) for y in range(n_y)]


def position_of(device, n_col):
    n_y = n_col // N_X
    x, y = device // n_y, device % n_y
    return x * n_y + jnp.where(x % 2 == 0, y, n_y - 1 - y)


def exchange(sent):
    return lax.all_to_all(
        sent, "col", split_axis=0, concat_axis=0, tiled=True, axis_index_groups=[exchange_order(sent.shape[0])]
    )


def routes(rows, cols, count, n_col):
    slots = rows.shape[0]
    live = jnp.arange(slots, dtype=jnp.int32) < count
    blocks = jnp.arange(n_col * BPD, dtype=jnp.int32)
    hits = (rows[None, :] == blocks[:, None]) & live[None, :]
    marked = jnp.any(hits, axis=1).astype(jnp.int32).reshape(n_col, BPD)
    local = jnp.arange(BPD, dtype=jnp.int32)
    rank = jnp.sum(marked[:, None, :] * (local[None, None, :] < local[None, :, None]), axis=2)
    slot_of = (position_of(jnp.arange(n_col, dtype=jnp.int32), n_col)[:, None] * TOUCH + rank).reshape(-1)
    slot = jnp.sum(jnp.where(hits, slot_of[:, None], 0), axis=0)
    slot = jnp.where(live, slot, n_col * TOUCH)
    row = lax.axis_index("row")
    owner, block = cols // BPD, cols % BPD
    far = (row // N_CORE - owner // N_CORE) % N_Z
    place = ((row % N_CORE != owner % N_CORE).astype(jnp.int32) * N_Z + far) * BPD + block
    return slot, place


def shards(tiles, tile_row, tile_col, tile_count, query_ids, damping):
    tiles, rows, cols, count = tiles[0, 0], tile_row[0, 0], tile_col[0, 0], tile_count[0, 0]
    tile = tiles.shape[1]
    queries = query_ids.shape[0]
    width = queries // STREAMS
    n_row, n_col = lax.axis_size("row"), lax.axis_size("col")
    col = lax.axis_index("col")

    def first_sent(round_index):
        return first_products(round_index, rows, cols, query_ids, count, col, tiles, n_col, n_row)

    sent = first_sent(0)
    got = exchange(sent)

    later_ids = after(query_ids, sent)
    home = later_ids // (BPD * tile) % n_col
    number = jnp.arange(queries, dtype=jnp.int32)
    same_home = home[:, None] == home[None, :]
    rank = jnp.sum((same_home & (number[None, :] < number[:, None])).astype(jnp.int32), axis=1)
    rounds = jnp.max(rank) // PLACES + 1

    def spread(round_index):
        place = rank - round_index * PLACES
        column = jnp.where((place >= 0) & (place < PLACES), position_of(home, n_col) * PLACES + place, -1)
        return (column[:, None] == jnp.arange(n_col * PLACES, dtype=jnp.int32)[None, :]).astype(BF16)

    slot, place = routes(after(rows, sent), cols, count, n_col)
    turned = turned_tiles(count.reshape(1), after(tiles, sent))
    first_spread = spread(0)
    got_ids = got[:, -ID_ROWS:, 0][:, :TOUCH].astype(jnp.int32).reshape(-1)
    sums = placed_sum(got_ids, after(got, turned, slot, place, first_spread), first_spread, width)

    def next_round(state):
        index, *sums = state
        got = exchange(first_sent(index))
        return index + 1, *placed_sum(got_ids, got, spread(index), width, sums)

    _, *sums = lax.while_loop(lambda state: state[0] < rounds, next_round, (jnp.int32(1), *sums))
    count = count.reshape(1)
    dampings = [
        jnp.broadcast_to(damping[stream * width : (stream + 1) * width][:, None], (width, tile))
        for stream in range(STREAMS)
    ]
    xparts = [None] * STREAMS
    owned, scores = sums, [None] * STREAMS
    for step in range(1, TERMS):
        for stream in range(STREAMS):
            if step == 1:
                mine = rounded(after(owned[stream], sent) if stream else owned[stream])
                xparts[stream] = column_parts(mine)
            sent, scores[stream] = products(
                step,
                slot,
                place,
                count,
                turned,
                xparts[stream],
                n_col,
                dampings[stream],
                owned[stream],
                scores[stream],
            )
            got = exchange(sent)
            if step + 1 < TERMS:
                mine, owned[stream] = owned_sum(got_ids, got, dampings[stream])
                xparts[stream] = column_parts(mine)
            elif stream + 1 < STREAMS:
                scores[stream] = ended_sum(step, got_ids, got, dampings[stream], scores[stream])
            else:
                total = last_sum(step, got_ids, got, dampings[stream], scores[stream], *scores[:-1])
    return total.reshape(BPD * tile, -1)


def solution(mesh):
    in_specs = (
        P("row", "col", None, None, None),
        P("row", "col", None),
        P("row", "col", None),
        P("row", "col"),
        P(),
        P(),
    )
    out_specs = P(("row", "col"), None)
    return jax.shard_map(shards, mesh=mesh, in_specs=in_specs, out_specs=out_specs, check_vma=False)
```

```python
import jax
import jax.numpy as jnp
from jax import lax
from jax.experimental import pallas as pl
from jax.experimental.pallas import tpu as pltpu
from jax.sharding import PartitionSpec as P


BPD = 8
TERMS = 4
TOUCH = 4
N_Z = 4
N_CORE = 2
N_X = 4
STREAMS = 2
PLACES = 24
ID_ROWS = 16
UNROLL = 16
FIRST_UNROLL = 8
CHUNK = 64
VMEM_LIMIT = 14 * 1024 * 1024

VMEM = pl.BlockSpec(memory_space=pltpu.VMEM)
HBM = pl.BlockSpec(memory_space=pltpu.HBM)
SMEM = pl.BlockSpec(memory_space=pltpu.SMEM)
PARAMS = pltpu.CompilerParams(vmem_limit_bytes=VMEM_LIMIT)
COVER = pl.CostEstimate(flops=int(8e9), bytes_accessed=int(40e6), transcendentals=0)
F32 = jnp.float32
BF16 = jnp.bfloat16


def power(damping_ref, step):
    damping = damping_ref[...]
    coef = damping
    for _ in range(step - 1):
        coef = coef * damping
    return coef


def multiply_tiles(slot_ref, place_ref, count, tile_ref, x_parts, acc_ref, x_ref):
    each = x_ref.shape[0] // len(x_parts)
    for part, part_ref in enumerate(x_parts):
        x_ref[part * each : (part + 1) * each] = part_ref[...]
    acc_ref[...] = jnp.zeros(acc_ref.shape, F32)

    def group(base):
        prods = []
        for lane in range(UNROLL):
            prods.append(
                jnp.dot(x_ref[place_ref[base + lane]], tile_ref[base + lane], preferred_element_type=F32)
            )
        for lane in range(UNROLL):
            slot = slot_ref[base + lane]
            acc_ref[slot] = acc_ref[slot] + prods[lane]

    def chunk_step(chunk, carry):
        for part in range(CHUNK // UNROLL):
            group(chunk * CHUNK + part * UNROLL)
        return carry

    lax.fori_loop(0, (count + CHUNK - 1) // CHUNK, chunk_step, 0)


def first_products(round_index, rows, cols, query_ids, count, col, tiles, n_col, n_row):
    slots, tile, _ = tiles.shape
    queries = query_ids.shape[0]
    col_blocks = n_row * BPD
    row_blocks = n_col * BPD
    spare = n_col * TOUCH
    sent_rows = TOUCH * PLACES
    tile_bits, col_bits, block_bits = (n.bit_length() - 1 for n in (tile, n_col, BPD))

    def body(info_ref, row_ref, col_ref, query_ref, tiles_ref, out_ref, *scratch):
        acc_ref, x_ref, tile_ref, id_rows_ref, asked_ref, has_ref, list_ref, mark_ref, slot_ref, id_ref, sems = scratch
        live, mine, first = info_ref[0], info_ref[1], info_ref[2] * PLACES

        def repeat(times, step, start=0, unroll=8):
            return lax.fori_loop(0, times, step, start, unroll=unroll)

        def clear(ref, value):
            def step(index, carry):
                ref[index] = value
                return carry

            repeat(ref.shape[0], step)

        def copy(index, lane):
            return pltpu.make_async_copy(tiles_ref.at[index], tile_ref.at[lane], sems.at[lane])

        def ask(query, found):
            node = query_ref[query]
            asked_ref[found] = node
            home = (node >> (tile_bits + block_bits)) & (n_col - 1)
            return found + (home == mine).astype(jnp.int32)

        asked = repeat(queries, ask)
        clear(has_ref, 0)
        x_ref[...] = jnp.zeros(x_ref.shape, BF16)
        place_of = lax.broadcasted_iota(jnp.int32, (PLACES, tile), 0)
        node_of = lax.broadcasted_iota(jnp.int32, (PLACES, tile), 1)

        def mark_query(place, carry):
            node = asked_ref[first + place]
            block = (node >> (tile_bits + block_bits + col_bits)) * BPD + ((node >> tile_bits) & (BPD - 1))
            here = (place_of == place) & (node_of == (node & (tile - 1)))
            x_ref[block] = jnp.where(here, 1.0, x_ref[block].astype(F32)).astype(BF16)
            has_ref[block] = 1
            return carry

        lax.fori_loop(0, jnp.clip(asked - first, 0, PLACES), mark_query, 0)

        def pick(index, found):
            list_ref[found] = index
            return found + jnp.where(index < live, has_ref[col_ref[index]], 0)

        found = repeat(slots, pick)

        def start(lane, carry):
            copy(list_ref[lane], lane).start()
            return carry

        lax.fori_loop(0, found, start, 0)
        clear(mark_ref, 0)

        def mark_row(index, carry):
            mark_ref[jnp.where(index < live, row_ref[index], row_blocks)] = 1
            return carry

        repeat(slots, mark_row)
        clear(id_ref, BPD)
        id_rows_ref[...] = jnp.full(id_rows_ref.shape, float(BPD), F32)

        def number_owner(owner, sent_to):
            rank = 0
            for block in range(BPD):
                marked = mark_ref[owner * BPD + block]
                slot_ref[owner * BPD + block] = sent_to * TOUCH + rank
                id_ref[sent_to * TOUCH + rank] = jnp.where(marked > 0, block, BPD)
                rank = rank + marked
            for place in range(TOUCH):
                number = id_ref[sent_to * TOUCH + place].astype(F32)
                id_rows_ref[sent_to, place : place + 1] = jnp.full((1, tile), number, F32)

        for sent_to, owner in enumerate(exchange_order(n_col)):
            number_owner(owner, sent_to)
        acc_ref[...] = jnp.zeros(acc_ref.shape, F32)

        def step(index, carry):
            prods, goes = [], []
            for lane in range(FIRST_UNROLL):
                at = index * FIRST_UNROLL + lane
                valid = at < found
                which = jnp.where(valid, list_ref[at], 0)

                @pl.when(valid)
                def _():
                    copy(which, at).wait()

                goes.append((at, which, valid))
            for at, which, valid in goes:
                prods.append(
                    lax.dot_general(
                        x_ref[col_ref[which]], tile_ref[at], (((1,), (1,)), ((), ())), preferred_element_type=F32
                    )
                )
            for (at, which, valid), prod in zip(goes, prods):
                slot = jnp.where(valid, slot_ref[row_ref[which]], spare)
                acc_ref[slot] = acc_ref[slot] + prod
            return carry

        lax.fori_loop(0, (found + FIRST_UNROLL - 1) // FIRST_UNROLL, step, 0)
        out_ref[:, :sent_rows] = acc_ref[:spare].reshape(n_col, sent_rows, tile).astype(BF16)
        out_ref[:, sent_rows:] = id_rows_ref[...].astype(BF16)

    info = jnp.stack([count, col, round_index]).astype(jnp.int32)
    return pl.pallas_call(
        body,
        out_shape=jax.ShapeDtypeStruct((n_col, sent_rows + ID_ROWS, tile), BF16),
        in_specs=[SMEM, SMEM, SMEM, SMEM, HBM],
        out_specs=VMEM,
        scratch_shapes=[
            pltpu.VMEM((spare + 1, PLACES, tile), F32),
            pltpu.VMEM((col_blocks, PLACES, tile), BF16),
            pltpu.VMEM(tiles.shape, tiles.dtype),
            pltpu.VMEM((n_col, ID_ROWS, tile), F32),
            pltpu.SMEM((queries,), jnp.int32),
            pltpu.SMEM((col_blocks,), jnp.int32),
            pltpu.SMEM((slots,), jnp.int32),
            pltpu.SMEM((row_blocks + 8,), jnp.int32),
            pltpu.SMEM((row_blocks,), jnp.int32),
            pltpu.SMEM((spare + 8,), jnp.int32),
            pltpu.SemaphoreType.DMA((slots,)),
        ],
        compiler_params=PARAMS,
        name="first_products",
    )(info, rows, cols, query_ids, pltpu.with_memory_space_constraint(tiles, pltpu.HBM))


def products(step, slots, places, count, turned, xparts, owners, damping, owned, scores):
    parts = len(xparts)
    each, width, tile = xparts[0].shape
    rows = TOUCH * width
    before = [] if step == 1 else [scores]

    def body(slot_ref, place_ref, count_ref, tiles_ref, *refs):
        x_refs, (damping_ref, owned_ref), refs = refs[:parts], refs[parts : parts + 2], refs[parts + 2 :]
        score_in, refs = refs[: len(before)], refs[len(before) :]
        out_ref, score_out, score_ref, score_sems, acc_ref, *scratch = refs
        for ref in score_in:
            pltpu.make_async_copy(ref, score_ref, score_sems.at[0]).start()
        multiply_tiles(slot_ref, place_ref, count_ref[0], tiles_ref, x_refs, acc_ref, *scratch)
        for ref in score_in:
            pltpu.make_async_copy(ref, score_ref, score_sems.at[0]).wait()
        if score_in:
            score_ref[...] = score_ref[...] + power(damping_ref, step - 1)[None] * owned_ref[...]
        else:
            score_ref[...] = owned_ref[...]
        leave = pltpu.make_async_copy(score_ref, score_out, score_sems.at[1])
        leave.start()
        out_ref[...] = acc_ref[: owners * TOUCH].astype(BF16).reshape(owners, rows, tile)
        leave.wait()

    return pl.pallas_call(
        body,
        out_shape=(
            jax.ShapeDtypeStruct((owners, rows, tile), BF16),
            pltpu.HBM((BPD, width, tile), F32),
        ),
        in_specs=[SMEM, SMEM, SMEM, VMEM] + [VMEM] * (parts + 2) + [HBM] * len(before),
        out_specs=(VMEM, HBM),
        scratch_shapes=[
            pltpu.VMEM((BPD, width, tile), F32),
            pltpu.SemaphoreType.DMA((2,)),
            pltpu.VMEM((owners * TOUCH + 1, width, tile), F32),
            pltpu.VMEM((parts * each, width, tile), BF16),
        ],
        compiler_params=PARAMS,
        name="products",
    )(
        slots,
        places,
        count,
        turned,
        *xparts,
        damping,
        owned,
        *[pltpu.with_memory_space_constraint(part, pltpu.HBM) for part in before],
    )


def turned_tiles(count, tiles):
    def body(count_ref, tiles_ref, out_ref):
        def group(index, carry):
            for lane in range(UNROLL):
                out_ref[index * UNROLL + lane] = jnp.transpose(tiles_ref[index * UNROLL + lane])
            return carry

        lax.fori_loop(0, (count_ref[0] + UNROLL - 1) // UNROLL, group, 0)

    return pl.pallas_call(
        body,
        out_shape=jax.ShapeDtypeStruct(tiles.shape, tiles.dtype),
        in_specs=[SMEM, VMEM],
        out_specs=VMEM,
        compiler_params=PARAMS,
        name="turned",
    )(count, tiles)


def summed(id_ref, got_ref, acc_ref):
    width = acc_ref.shape[1]
    acc_ref[...] = jnp.zeros(acc_ref.shape, F32)
    for source in range(got_ref.shape[0]):
        for place in range(TOUCH):
            block = id_ref[source * TOUCH + place]
            part = got_ref[source, place * width : (place + 1) * width].astype(F32)
            acc_ref[block] = acc_ref[block] + part


def owned_sum(ids, got, damping):
    width, tile = damping.shape

    def body(id_ref, got_ref, x_ref, out_ref, acc_ref):
        summed(id_ref, got_ref, acc_ref)
        owned = acc_ref[:BPD]
        x_ref[...] = owned.astype(BF16)
        out_ref[...] = owned

    return pl.pallas_call(
        body,
        out_shape=(
            jax.ShapeDtypeStruct((BPD, width, tile), BF16),
            jax.ShapeDtypeStruct((BPD, width, tile), F32),
        ),
        in_specs=[SMEM, VMEM],
        out_specs=(VMEM, VMEM),
        scratch_shapes=[pltpu.VMEM((BPD + 1, width, tile), F32)],
        compiler_params=PARAMS,
        cost_estimate=COVER,
        name="owned",
    )(ids, got)


def placed_sum(ids, got, spread, width, before=()):
    sources, _, tile = got.shape
    queries, columns = spread.shape
    streams = queries // width

    def body(id_ref, got_ref, spread_ref, *refs):
        whole_refs, out_refs, piece_ref = refs[: len(before)], refs[len(before) : -1], refs[-1]
        piece_ref[...] = jnp.zeros(piece_ref.shape, F32)
        for source in range(sources):
            part = got_ref[source].astype(F32)
            for place in range(TOUCH):
                block = id_ref[source * TOUCH + place]
                piece_ref[block, source * PLACES : (source + 1) * PLACES] = part[
                    place * PLACES : (place + 1) * PLACES
                ]
        for block in range(BPD):
            owned = jnp.dot(spread_ref[...], piece_ref[block].astype(BF16), preferred_element_type=F32)
            for stream in range(streams):
                mine = owned[stream * width : (stream + 1) * width]
                if whole_refs:
                    mine = mine + whole_refs[stream][block]
                out_refs[stream][block] = mine

    shape = (BPD, width, tile)
    return pl.pallas_call(
        body,
        out_shape=[jax.ShapeDtypeStruct(shape, F32)] * streams,
        in_specs=[SMEM] + [VMEM] * (2 + len(before)),
        out_specs=[VMEM] * streams,
        scratch_shapes=[pltpu.VMEM((BPD + 1, columns, tile), F32)],
        compiler_params=PARAMS,
        name="placed",
    )(ids, got, spread, *before)


def rounded(whole):
    def body(whole_ref, out_ref):
        out_ref[...] = whole_ref[...].astype(BF16)

    return pl.pallas_call(
        body,
        out_shape=jax.ShapeDtypeStruct(whole.shape, BF16),
        in_specs=[VMEM],
        out_specs=VMEM,
        compiler_params=PARAMS,
        cost_estimate=COVER,
        name="rounded",
    )(whole)


def ended_sum(step, ids, got, damping, scores):
    width, tile = damping.shape

    def body(id_ref, got_ref, damping_ref, score_ref, out_ref, acc_ref):
        summed(id_ref, got_ref, acc_ref)
        out_ref[...] = score_ref[...] + power(damping_ref, step)[None] * acc_ref[:BPD]

    return pl.pallas_call(
        body,
        out_shape=jax.ShapeDtypeStruct((BPD, width, tile), F32),
        in_specs=[SMEM] + [VMEM] * 3,
        out_specs=VMEM,
        scratch_shapes=[pltpu.VMEM((BPD + 1, width, tile), F32)],
        compiler_params=PARAMS,
        name="ended",
    )(ids, got, damping, scores)


def last_sum(step, ids, got, damping, scores, *done):
    width, tile = damping.shape
    queries = sum(part.shape[1] for part in done) + width

    def body(id_ref, got_ref, damping_ref, score_ref, *refs):
        done_refs, (out_ref, acc_ref, block_ref, sems) = refs[:-4], refs[-4:]
        summed(id_ref, got_ref, acc_ref)
        coef = power(damping_ref, step)
        leaving = []
        for block in range(BPD):
            mine = score_ref[block] + coef * acc_ref[block]
            rows = [part[block] for part in done_refs] + [mine]
            block_ref[block] = jnp.transpose(jnp.concatenate(rows, axis=0))
            leaving.append(pltpu.make_async_copy(block_ref.at[block], out_ref.at[block], sems.at[block]))
            leaving[-1].start()
        for copy in leaving:
            copy.wait()

    return pl.pallas_call(
        body,
        out_shape=pltpu.HBM((BPD, tile, queries), F32),
        in_specs=[SMEM] + [VMEM] * (3 + len(done)),
        out_specs=HBM,
        scratch_shapes=[
            pltpu.VMEM((BPD + 1, width, tile), F32),
            pltpu.VMEM((BPD, tile, queries), F32),
            pltpu.SemaphoreType.DMA((BPD,)),
        ],
        compiler_params=PARAMS,
        name="last",
    )(ids, got, damping, scores, *done)


def row_shift(dz, dcore):
    return [
        (z * N_CORE + core, (z + dz) % N_Z * N_CORE + (core + dcore) % N_CORE)
        for z in range(N_Z)
        for core in range(N_CORE)
    ]


def column_parts(mine):
    same = [mine] + [lax.ppermute(mine, "row", row_shift(dz, 0)) for dz in range(1, N_Z)]
    other = [lax.ppermute(part, "row", row_shift(0, 1)) for part in same]
    return same + other


def after(value, *others):
    return lax.optimization_barrier((value, *others))[0]


def exchange_order(n_col):
    n_y = n_col // N_X
    return [x * n_y + (y if x % 2 == 0 else n_y - 1 - y) for x in range(N_X) for y in range(n_y)]


def position_of(device, n_col):
    n_y = n_col // N_X
    x, y = device // n_y, device % n_y
    return x * n_y + jnp.where(x % 2 == 0, y, n_y - 1 - y)


def exchange(sent):
    return lax.all_to_all(
        sent, "col", split_axis=0, concat_axis=0, tiled=True, axis_index_groups=[exchange_order(sent.shape[0])]
    )


def routes(rows, cols, count, n_col):
    slots = rows.shape[0]
    live = jnp.arange(slots, dtype=jnp.int32) < count
    blocks = jnp.arange(n_col * BPD, dtype=jnp.int32)
    hits = (rows[None, :] == blocks[:, None]) & live[None, :]
    marked = jnp.any(hits, axis=1).astype(jnp.int32).reshape(n_col, BPD)
    local = jnp.arange(BPD, dtype=jnp.int32)
    rank = jnp.sum(marked[:, None, :] * (local[None, None, :] < local[None, :, None]), axis=2)
    slot_of = (position_of(jnp.arange(n_col, dtype=jnp.int32), n_col)[:, None] * TOUCH + rank).reshape(-1)
    slot = jnp.sum(jnp.where(hits, slot_of[:, None], 0), axis=0)
    slot = jnp.where(live, slot, n_col * TOUCH)
    row = lax.axis_index("row")
    owner, block = cols // BPD, cols % BPD
    far = (row // N_CORE - owner // N_CORE) % N_Z
    place = ((row % N_CORE != owner % N_CORE).astype(jnp.int32) * N_Z + far) * BPD + block
    return slot, place


def shards(tiles, tile_row, tile_col, tile_count, query_ids, damping):
    tiles, rows, cols, count = tiles[0, 0], tile_row[0, 0], tile_col[0, 0], tile_count[0, 0]
    tile = tiles.shape[1]
    queries = query_ids.shape[0]
    width = queries // STREAMS
    n_row, n_col = lax.axis_size("row"), lax.axis_size("col")
    col = lax.axis_index("col")

    def first_sent(round_index):
        return first_products(round_index, rows, cols, query_ids, count, col, tiles, n_col, n_row)

    sent = first_sent(0)
    got = exchange(sent)

    later_ids = after(query_ids, sent)
    home = later_ids // (BPD * tile) % n_col
    number = jnp.arange(queries, dtype=jnp.int32)
    same_home = home[:, None] == home[None, :]
    rank = jnp.sum((same_home & (number[None, :] < number[:, None])).astype(jnp.int32), axis=1)
    rounds = jnp.max(rank) // PLACES + 1

    def spread(round_index):
        place = rank - round_index * PLACES
        column = jnp.where((place >= 0) & (place < PLACES), position_of(home, n_col) * PLACES + place, -1)
        return (column[:, None] == jnp.arange(n_col * PLACES, dtype=jnp.int32)[None, :]).astype(BF16)

    slot, place = routes(after(rows, sent), cols, count, n_col)
    turned = turned_tiles(count.reshape(1), after(tiles, sent))
    first_spread = spread(0)
    got_ids = got[:, -ID_ROWS:, 0][:, :TOUCH].astype(jnp.int32).reshape(-1)
    sums = placed_sum(got_ids, after(got, turned, slot, place, first_spread), first_spread, width)

    def next_round(state):
        index, *sums = state
        got = exchange(first_sent(index))
        return index + 1, *placed_sum(got_ids, got, spread(index), width, sums)

    _, *sums = lax.while_loop(lambda state: state[0] < rounds, next_round, (jnp.int32(1), *sums))
    count = count.reshape(1)
    dampings = [
        jnp.broadcast_to(damping[stream * width : (stream + 1) * width][:, None], (width, tile))
        for stream in range(STREAMS)
    ]
    xparts = [None] * STREAMS
    owned, scores = sums, [None] * STREAMS
    for step in range(1, TERMS):
        for stream in range(STREAMS):
            if step == 1:
                mine = rounded(after(owned[stream], sent) if stream else owned[stream])
                xparts[stream] = column_parts(mine)
            sent, scores[stream] = products(
                step,
                slot,
                place,
                count,
                turned,
                xparts[stream],
                n_col,
                dampings[stream],
                owned[stream],
                scores[stream],
            )
            got = exchange(sent)
            if step + 1 < TERMS:
                mine, owned[stream] = owned_sum(got_ids, got, dampings[stream])
                xparts[stream] = column_parts(mine)
            elif stream + 1 < STREAMS:
                scores[stream] = ended_sum(step, got_ids, got, dampings[stream], scores[stream])
            else:
                total = last_sum(step, got_ids, got, dampings[stream], scores[stream], *scores[:-1])
    return total.reshape(BPD * tile, -1)


def solution(mesh):
    in_specs = (
        P("row", "col", None, None, None),
        P("row", "col", None),
        P("row", "col", None),
        P("row", "col"),
        P(),
        P(),
    )
    out_specs = P(("row", "col"), None)
    return jax.shard_map(shards, mesh=mesh, in_specs=in_specs, out_specs=out_specs, check_vma=False)
```

```python
import jax
import jax.numpy as jnp
from jax import lax
from jax.experimental import pallas as pl
from jax.experimental.pallas import tpu as pltpu
from jax.sharding import PartitionSpec as P


BPD = 8
TERMS = 4
TOUCH = 4
N_Z = 4
N_CORE = 2
N_X = 4
STREAMS = 2
PLACES = 24
ID_ROWS = 16
UNROLL = 16
FIRST_UNROLL = 8
CHUNK = 64
VMEM_LIMIT = 14 * 1024 * 1024

VMEM = pl.BlockSpec(memory_space=pltpu.VMEM)
HBM = pl.BlockSpec(memory_space=pltpu.HBM)
SMEM = pl.BlockSpec(memory_space=pltpu.SMEM)
PARAMS = pltpu.CompilerParams(vmem_limit_bytes=VMEM_LIMIT)
COVER = pl.CostEstimate(flops=int(8e9), bytes_accessed=int(40e6), transcendentals=0)
F32 = jnp.float32
BF16 = jnp.bfloat16


def power(damping_ref, step):
    damping = damping_ref[...]
    coef = damping
    for _ in range(step - 1):
        coef = coef * damping
    return coef


def multiply_tiles(slot_ref, place_ref, count, tile_ref, x_parts, acc_ref, x_ref, aside):
    each = x_ref.shape[0] // len(x_parts)
    for part, part_ref in enumerate(x_parts):
        x_ref[part * each : (part + 1) * each] = part_ref[...]
    acc_ref[...] = jnp.zeros(acc_ref.shape, F32)

    def group(base):
        prods = []
        for lane in range(UNROLL):
            prods.append(
                jnp.dot(x_ref[place_ref[base + lane]], tile_ref[base + lane], preferred_element_type=F32)
            )
        for lane in range(UNROLL):
            slot = slot_ref[base + lane]
            acc_ref[slot] = acc_ref[slot] + prods[lane]

    def chunk_step(chunk, carry):
        for part in range(CHUNK // UNROLL):
            group(chunk * CHUNK + part * UNROLL)
        pl.when(chunk == 0)(aside)
        return carry

    lax.fori_loop(0, jnp.maximum((count + CHUNK - 1) // CHUNK, 1), chunk_step, 0)


def first_products(round_index, rows, cols, query_ids, count, col, tiles, n_col, n_row):
    slots, tile, _ = tiles.shape
    queries = query_ids.shape[0]
    col_blocks = n_row * BPD
    row_blocks = n_col * BPD
    spare = n_col * TOUCH
    sent_rows = TOUCH * PLACES
    tile_bits, col_bits, block_bits = (n.bit_length() - 1 for n in (tile, n_col, BPD))

    def body(info_ref, row_ref, col_ref, query_ref, tiles_ref, out_ref, *scratch):
        acc_ref, x_ref, tile_ref, id_rows_ref, asked_ref, has_ref, list_ref, mark_ref, slot_ref, id_ref, sems = scratch
        live, mine, first = info_ref[0], info_ref[1], info_ref[2] * PLACES

        def repeat(times, step, start=0, unroll=8):
            return lax.fori_loop(0, times, step, start, unroll=unroll)

        def clear(ref, value):
            def step(index, carry):
                ref[index] = value
                return carry

            repeat(ref.shape[0], step)

        def copy(index, lane):
            return pltpu.make_async_copy(tiles_ref.at[index], tile_ref.at[lane], sems.at[lane])

        def ask(query, found):
            node = query_ref[query]
            asked_ref[found] = node
            home = (node >> (tile_bits + block_bits)) & (n_col - 1)
            return found + (home == mine).astype(jnp.int32)

        asked = repeat(queries, ask)
        clear(has_ref, 0)
        x_ref[...] = jnp.zeros(x_ref.shape, BF16)
        place_of = lax.broadcasted_iota(jnp.int32, (PLACES, tile), 0)
        node_of = lax.broadcasted_iota(jnp.int32, (PLACES, tile), 1)

        def mark_query(place, carry):
            node = asked_ref[first + place]
            block = (node >> (tile_bits + block_bits + col_bits)) * BPD + ((node >> tile_bits) & (BPD - 1))
            here = (place_of == place) & (node_of == (node & (tile - 1)))
            x_ref[block] = jnp.where(here, 1.0, x_ref[block].astype(F32)).astype(BF16)
            has_ref[block] = 1
            return carry

        lax.fori_loop(0, jnp.clip(asked - first, 0, PLACES), mark_query, 0)

        def pick(index, found):
            list_ref[found] = index
            return found + jnp.where(index < live, has_ref[col_ref[index]], 0)

        found = repeat(slots, pick)

        def start(lane, carry):
            copy(list_ref[lane], lane).start()
            return carry

        lax.fori_loop(0, found, start, 0)
        clear(mark_ref, 0)

        def mark_row(index, carry):
            mark_ref[jnp.where(index < live, row_ref[index], row_blocks)] = 1
            return carry

        repeat(slots, mark_row)
        clear(id_ref, BPD)
        id_rows_ref[...] = jnp.full(id_rows_ref.shape, float(BPD), F32)

        def number_owner(owner, sent_to):
            rank = 0
            for block in range(BPD):
                marked = mark_ref[owner * BPD + block]
                slot_ref[owner * BPD + block] = sent_to * TOUCH + rank
                id_ref[sent_to * TOUCH + rank] = jnp.where(marked > 0, block, BPD)
                rank = rank + marked
            for place in range(TOUCH):
                number = id_ref[sent_to * TOUCH + place].astype(F32)
                id_rows_ref[sent_to, place : place + 1] = jnp.full((1, tile), number, F32)

        for sent_to, owner in enumerate(exchange_order(n_col)):
            number_owner(owner, sent_to)
        acc_ref[...] = jnp.zeros(acc_ref.shape, F32)

        def step(index, carry):
            prods, goes = [], []
            for lane in range(FIRST_UNROLL):
                at = index * FIRST_UNROLL + lane
                valid = at < found
                which = jnp.where(valid, list_ref[at], 0)

                @pl.when(valid)
                def _():
                    copy(which, at).wait()

                goes.append((at, which, valid))
            for at, which, valid in goes:
                prods.append(
                    lax.dot_general(
                        x_ref[col_ref[which]], tile_ref[at], (((1,), (1,)), ((), ())), preferred_element_type=F32
                    )
                )
            for (at, which, valid), prod in zip(goes, prods):
                slot = jnp.where(valid, slot_ref[row_ref[which]], spare)
                acc_ref[slot] = acc_ref[slot] + prod
            return carry

        lax.fori_loop(0, (found + FIRST_UNROLL - 1) // FIRST_UNROLL, step, 0)
        out_ref[:, :sent_rows] = acc_ref[:spare].reshape(n_col, sent_rows, tile).astype(BF16)
        out_ref[:, sent_rows:] = id_rows_ref[...].astype(BF16)

    info = jnp.stack([count, col, round_index]).astype(jnp.int32)
    return pl.pallas_call(
        body,
        out_shape=jax.ShapeDtypeStruct((n_col, sent_rows + ID_ROWS, tile), BF16),
        in_specs=[SMEM, SMEM, SMEM, SMEM, HBM],
        out_specs=VMEM,
        scratch_shapes=[
            pltpu.VMEM((spare + 1, PLACES, tile), F32),
            pltpu.VMEM((col_blocks, PLACES, tile), BF16),
            pltpu.VMEM(tiles.shape, tiles.dtype),
            pltpu.VMEM((n_col, ID_ROWS, tile), F32),
            pltpu.SMEM((queries,), jnp.int32),
            pltpu.SMEM((col_blocks,), jnp.int32),
            pltpu.SMEM((slots,), jnp.int32),
            pltpu.SMEM((row_blocks + 8,), jnp.int32),
            pltpu.SMEM((row_blocks,), jnp.int32),
            pltpu.SMEM((spare + 8,), jnp.int32),
            pltpu.SemaphoreType.DMA((slots,)),
        ],
        compiler_params=PARAMS,
        name="first_products",
    )(info, rows, cols, query_ids, pltpu.with_memory_space_constraint(tiles, pltpu.HBM))


def products(step, slots, places, count, turned, xparts, owners, damping, owned, scores):
    parts = len(xparts)
    each, width, tile = xparts[0].shape
    rows = TOUCH * width
    before = [] if step == 1 else [scores]

    def body(slot_ref, place_ref, count_ref, tiles_ref, *refs):
        x_refs, (damping_ref, owned_ref), refs = refs[:parts], refs[parts : parts + 2], refs[parts + 2 :]
        score_in, refs = refs[: len(before)], refs[len(before) :]
        out_ref, score_out, score_ref, score_sems, acc_ref, *scratch = refs
        for ref in score_in:
            pltpu.make_async_copy(ref, score_ref, score_sems.at[0]).start()
        leave = pltpu.make_async_copy(score_ref, score_out, score_sems.at[1])

        def add_scores():
            for ref in score_in:
                pltpu.make_async_copy(ref, score_ref, score_sems.at[0]).wait()
            if score_in:
                score_ref[...] = score_ref[...] + power(damping_ref, step - 1)[None] * owned_ref[...]
            else:
                score_ref[...] = owned_ref[...]
            leave.start()

        multiply_tiles(slot_ref, place_ref, count_ref[0], tiles_ref, x_refs, acc_ref, *scratch, add_scores)
        out_ref[...] = acc_ref[: owners * TOUCH].astype(BF16).reshape(owners, rows, tile)
        leave.wait()

    return pl.pallas_call(
        body,
        out_shape=(
            jax.ShapeDtypeStruct((owners, rows, tile), BF16),
            pltpu.HBM((BPD, width, tile), F32),
        ),
        in_specs=[SMEM, SMEM, SMEM, VMEM] + [VMEM] * (parts + 2) + [HBM] * len(before),
        out_specs=(VMEM, HBM),
        scratch_shapes=[
            pltpu.VMEM((BPD, width, tile), F32),
            pltpu.SemaphoreType.DMA((2,)),
            pltpu.VMEM((owners * TOUCH + 1, width, tile), F32),
            pltpu.VMEM((parts * each, width, tile), BF16),
        ],
        compiler_params=PARAMS,
        name="products",
    )(
        slots,
        places,
        count,
        turned,
        *xparts,
        damping,
        owned,
        *[pltpu.with_memory_space_constraint(part, pltpu.HBM) for part in before],
    )


def turned_tiles(count, tiles):
    def body(count_ref, tiles_ref, out_ref):
        def group(index, carry):
            for lane in range(UNROLL):
                out_ref[index * UNROLL + lane] = jnp.transpose(tiles_ref[index * UNROLL + lane])
            return carry

        lax.fori_loop(0, (count_ref[0] + UNROLL - 1) // UNROLL, group, 0)

    return pl.pallas_call(
        body,
        out_shape=jax.ShapeDtypeStruct(tiles.shape, tiles.dtype),
        in_specs=[SMEM, VMEM],
        out_specs=VMEM,
        compiler_params=PARAMS,
        name="turned",
    )(count, tiles)


def summed(id_ref, got_ref, acc_ref):
    width = acc_ref.shape[1]
    acc_ref[...] = jnp.zeros(acc_ref.shape, F32)
    for source in range(got_ref.shape[0]):
        for place in range(TOUCH):
            block = id_ref[source * TOUCH + place]
            part = got_ref[source, place * width : (place + 1) * width].astype(F32)
            acc_ref[block] = acc_ref[block] + part


def owned_sum(ids, got, damping):
    width, tile = damping.shape

    def body(id_ref, got_ref, x_ref, out_ref, acc_ref):
        summed(id_ref, got_ref, acc_ref)
        owned = acc_ref[:BPD]
        x_ref[...] = owned.astype(BF16)
        out_ref[...] = owned

    return pl.pallas_call(
        body,
        out_shape=(
            jax.ShapeDtypeStruct((BPD, width, tile), BF16),
            jax.ShapeDtypeStruct((BPD, width, tile), F32),
        ),
        in_specs=[SMEM, VMEM],
        out_specs=(VMEM, VMEM),
        scratch_shapes=[pltpu.VMEM((BPD + 1, width, tile), F32)],
        compiler_params=PARAMS,
        cost_estimate=COVER,
        name="owned",
    )(ids, got)


def placed_sum(ids, got, spread, width, before=()):
    sources, _, tile = got.shape
    queries, columns = spread.shape
    streams = queries // width

    def body(id_ref, got_ref, spread_ref, *refs):
        whole_refs, out_refs, piece_ref = refs[: len(before)], refs[len(before) : -1], refs[-1]
        piece_ref[...] = jnp.zeros(piece_ref.shape, F32)
        for source in range(sources):
            part = got_ref[source].astype(F32)
            for place in range(TOUCH):
                block = id_ref[source * TOUCH + place]
                piece_ref[block, source * PLACES : (source + 1) * PLACES] = part[
                    place * PLACES : (place + 1) * PLACES
                ]
        for block in range(BPD):
            owned = jnp.dot(spread_ref[...], piece_ref[block].astype(BF16), preferred_element_type=F32)
            for stream in range(streams):
                mine = owned[stream * width : (stream + 1) * width]
                if whole_refs:
                    mine = mine + whole_refs[stream][block]
                out_refs[stream][block] = mine

    shape = (BPD, width, tile)
    return pl.pallas_call(
        body,
        out_shape=[jax.ShapeDtypeStruct(shape, F32)] * streams,
        in_specs=[SMEM] + [VMEM] * (2 + len(before)),
        out_specs=[VMEM] * streams,
        scratch_shapes=[pltpu.VMEM((BPD + 1, columns, tile), F32)],
        compiler_params=PARAMS,
        name="placed",
    )(ids, got, spread, *before)


def rounded(whole):
    def body(whole_ref, out_ref):
        out_ref[...] = whole_ref[...].astype(BF16)

    return pl.pallas_call(
        body,
        out_shape=jax.ShapeDtypeStruct(whole.shape, BF16),
        in_specs=[VMEM],
        out_specs=VMEM,
        compiler_params=PARAMS,
        cost_estimate=COVER,
        name="rounded",
    )(whole)


def ended_sum(step, ids, got, damping, scores):
    width, tile = damping.shape

    def body(id_ref, got_ref, damping_ref, score_ref, out_ref, acc_ref):
        summed(id_ref, got_ref, acc_ref)
        out_ref[...] = score_ref[...] + power(damping_ref, step)[None] * acc_ref[:BPD]

    return pl.pallas_call(
        body,
        out_shape=jax.ShapeDtypeStruct((BPD, width, tile), F32),
        in_specs=[SMEM] + [VMEM] * 3,
        out_specs=VMEM,
        scratch_shapes=[pltpu.VMEM((BPD + 1, width, tile), F32)],
        compiler_params=PARAMS,
        name="ended",
    )(ids, got, damping, scores)


def last_sum(step, ids, got, damping, scores, *done):
    width, tile = damping.shape
    queries = sum(part.shape[1] for part in done) + width

    def body(id_ref, got_ref, damping_ref, score_ref, *refs):
        done_refs, (out_ref, acc_ref, block_ref, sems) = refs[:-4], refs[-4:]
        summed(id_ref, got_ref, acc_ref)
        coef = power(damping_ref, step)
        leaving = []
        for block in range(BPD):
            mine = score_ref[block] + coef * acc_ref[block]
            rows = [part[block] for part in done_refs] + [mine]
            block_ref[block] = jnp.transpose(jnp.concatenate(rows, axis=0))
            leaving.append(pltpu.make_async_copy(block_ref.at[block], out_ref.at[block], sems.at[block]))
            leaving[-1].start()
        for copy in leaving:
            copy.wait()

    return pl.pallas_call(
        body,
        out_shape=pltpu.HBM((BPD, tile, queries), F32),
        in_specs=[SMEM] + [VMEM] * (3 + len(done)),
        out_specs=HBM,
        scratch_shapes=[
            pltpu.VMEM((BPD + 1, width, tile), F32),
            pltpu.VMEM((BPD, tile, queries), F32),
            pltpu.SemaphoreType.DMA((BPD,)),
        ],
        compiler_params=PARAMS,
        name="last",
    )(ids, got, damping, scores, *done)


def row_shift(dz, dcore):
    return [
        (z * N_CORE + core, (z + dz) % N_Z * N_CORE + (core + dcore) % N_CORE)
        for z in range(N_Z)
        for core in range(N_CORE)
    ]


def column_parts(mine):
    same = [mine] + [lax.ppermute(mine, "row", row_shift(dz, 0)) for dz in range(1, N_Z)]
    other = [lax.ppermute(part, "row", row_shift(0, 1)) for part in same]
    return same + other


def after(value, *others):
    return lax.optimization_barrier((value, *others))[0]


def exchange_order(n_col):
    n_y = n_col // N_X
    return [x * n_y + (y if x % 2 == 0 else n_y - 1 - y) for x in range(N_X) for y in range(n_y)]


def position_of(device, n_col):
    n_y = n_col // N_X
    x, y = device // n_y, device % n_y
    return x * n_y + jnp.where(x % 2 == 0, y, n_y - 1 - y)


def exchange(sent):
    return lax.all_to_all(
        sent, "col", split_axis=0, concat_axis=0, tiled=True, axis_index_groups=[exchange_order(sent.shape[0])]
    )


def routes(rows, cols, count, n_col):
    slots = rows.shape[0]
    live = jnp.arange(slots, dtype=jnp.int32) < count
    blocks = jnp.arange(n_col * BPD, dtype=jnp.int32)
    hits = (rows[None, :] == blocks[:, None]) & live[None, :]
    marked = jnp.any(hits, axis=1).astype(jnp.int32).reshape(n_col, BPD)
    local = jnp.arange(BPD, dtype=jnp.int32)
    rank = jnp.sum(marked[:, None, :] * (local[None, None, :] < local[None, :, None]), axis=2)
    slot_of = (position_of(jnp.arange(n_col, dtype=jnp.int32), n_col)[:, None] * TOUCH + rank).reshape(-1)
    slot = jnp.sum(jnp.where(hits, slot_of[:, None], 0), axis=0)
    slot = jnp.where(live, slot, n_col * TOUCH)
    row = lax.axis_index("row")
    owner, block = cols // BPD, cols % BPD
    far = (row // N_CORE - owner // N_CORE) % N_Z
    place = ((row % N_CORE != owner % N_CORE).astype(jnp.int32) * N_Z + far) * BPD + block
    return slot, place


def shards(tiles, tile_row, tile_col, tile_count, query_ids, damping):
    tiles, rows, cols, count = tiles[0, 0], tile_row[0, 0], tile_col[0, 0], tile_count[0, 0]
    tile = tiles.shape[1]
    queries = query_ids.shape[0]
    width = queries // STREAMS
    n_row, n_col = lax.axis_size("row"), lax.axis_size("col")
    col = lax.axis_index("col")

    def first_sent(round_index):
        return first_products(round_index, rows, cols, query_ids, count, col, tiles, n_col, n_row)

    sent = first_sent(0)
    got = exchange(sent)

    later_ids = after(query_ids, sent)
    home = later_ids // (BPD * tile) % n_col
    number = jnp.arange(queries, dtype=jnp.int32)
    same_home = home[:, None] == home[None, :]
    rank = jnp.sum((same_home & (number[None, :] < number[:, None])).astype(jnp.int32), axis=1)
    rounds = jnp.max(rank) // PLACES + 1

    def spread(round_index):
        place = rank - round_index * PLACES
        column = jnp.where((place >= 0) & (place < PLACES), position_of(home, n_col) * PLACES + place, -1)
        return (column[:, None] == jnp.arange(n_col * PLACES, dtype=jnp.int32)[None, :]).astype(BF16)

    slot, place = routes(after(rows, sent), cols, count, n_col)
    turned = turned_tiles(count.reshape(1), after(tiles, sent))
    first_spread = spread(0)
    got_ids = got[:, -ID_ROWS:, 0][:, :TOUCH].astype(jnp.int32).reshape(-1)
    sums = placed_sum(got_ids, after(got, turned, slot, place, first_spread), first_spread, width)

    def next_round(state):
        index, *sums = state
        got = exchange(first_sent(index))
        return index + 1, *placed_sum(got_ids, got, spread(index), width, sums)

    _, *sums = lax.while_loop(lambda state: state[0] < rounds, next_round, (jnp.int32(1), *sums))
    count = count.reshape(1)
    dampings = [
        jnp.broadcast_to(damping[stream * width : (stream + 1) * width][:, None], (width, tile))
        for stream in range(STREAMS)
    ]
    xparts = [None] * STREAMS
    owned, scores = sums, [None] * STREAMS
    for step in range(1, TERMS):
        for stream in range(STREAMS):
            if step == 1:
                mine = rounded(after(owned[stream], sent) if stream else owned[stream])
                xparts[stream] = column_parts(mine)
            sent, scores[stream] = products(
                step,
                slot,
                place,
                count,
                turned,
                xparts[stream],
                n_col,
                dampings[stream],
                owned[stream],
                scores[stream],
            )
            got = exchange(sent)
            if step + 1 < TERMS:
                mine, owned[stream] = owned_sum(got_ids, got, dampings[stream])
                xparts[stream] = column_parts(mine)
            elif stream + 1 < STREAMS:
                scores[stream] = ended_sum(step, got_ids, got, dampings[stream], scores[stream])
            else:
                total = last_sum(step, got_ids, got, dampings[stream], scores[stream], *scores[:-1])
    return total.reshape(BPD * tile, -1)


def solution(mesh):
    in_specs = (
        P("row", "col", None, None, None),
        P("row", "col", None),
        P("row", "col", None),
        P("row", "col"),
        P(),
        P(),
    )
    out_specs = P(("row", "col"), None)
    return jax.shard_map(shards, mesh=mesh, in_specs=in_specs, out_specs=out_specs, check_vma=False)
```

```python
import jax
import jax.numpy as jnp
from jax import lax
from jax.experimental import pallas as pl
from jax.experimental.pallas import tpu as pltpu
from jax.sharding import PartitionSpec as P


BPD = 8
TERMS = 4
TOUCH = 4
N_Z = 4
N_CORE = 2
N_X = 4
STREAMS = 2
PLACES = 24
ID_ROWS = 16
UNROLL = 16
FIRST_UNROLL = 16
CHUNK = 64
VMEM_LIMIT = 14 * 1024 * 1024

VMEM = pl.BlockSpec(memory_space=pltpu.VMEM)
HBM = pl.BlockSpec(memory_space=pltpu.HBM)
SMEM = pl.BlockSpec(memory_space=pltpu.SMEM)
PARAMS = pltpu.CompilerParams(vmem_limit_bytes=VMEM_LIMIT)
COVER = pl.CostEstimate(flops=int(8e9), bytes_accessed=int(40e6), transcendentals=0)
F32 = jnp.float32
BF16 = jnp.bfloat16


def power(damping_ref, step):
    damping = damping_ref[...]
    coef = damping
    for _ in range(step - 1):
        coef = coef * damping
    return coef


def multiply_tiles(slot_ref, place_ref, count, tile_ref, x_parts, acc_ref, x_ref, aside):
    each = x_ref.shape[0] // len(x_parts)
    for part, part_ref in enumerate(x_parts):
        x_ref[part * each : (part + 1) * each] = part_ref[...]
    acc_ref[...] = jnp.zeros(acc_ref.shape, F32)

    def group(base):
        prods = []
        for lane in range(UNROLL):
            prods.append(
                jnp.dot(x_ref[place_ref[base + lane]], tile_ref[base + lane], preferred_element_type=F32)
            )
        for lane in range(UNROLL):
            slot = slot_ref[base + lane]
            acc_ref[slot] = acc_ref[slot] + prods[lane]

    def chunk_step(chunk, carry):
        for part in range(CHUNK // UNROLL):
            group(chunk * CHUNK + part * UNROLL)
        pl.when(chunk == 0)(aside)
        return carry

    lax.fori_loop(0, jnp.maximum((count + CHUNK - 1) // CHUNK, 1), chunk_step, 0)


def first_products(round_index, rows, cols, query_ids, count, col, tiles, n_col, n_row):
    slots, tile, _ = tiles.shape
    queries = query_ids.shape[0]
    col_blocks = n_row * BPD
    row_blocks = n_col * BPD
    spare = n_col * TOUCH
    sent_rows = TOUCH * PLACES
    tile_bits, col_bits, block_bits = (n.bit_length() - 1 for n in (tile, n_col, BPD))

    def body(info_ref, row_ref, col_ref, query_ref, tiles_ref, out_ref, *scratch):
        acc_ref, x_ref, tile_ref, id_rows_ref, asked_ref, has_ref, list_ref, mark_ref, slot_ref, id_ref, sems = scratch
        live, mine, first = info_ref[0], info_ref[1], info_ref[2] * PLACES

        def repeat(times, step, start=0, unroll=32):
            return lax.fori_loop(0, times, step, start, unroll=unroll)

        def clear(ref, value):
            def step(index, carry):
                ref[index] = value
                return carry

            repeat(ref.shape[0], step, unroll=8)

        def copy(index, lane):
            return pltpu.make_async_copy(tiles_ref.at[index], tile_ref.at[lane], sems.at[lane])

        def ask(query, found):
            node = query_ref[query]
            asked_ref[found] = node
            home = (node >> (tile_bits + block_bits)) & (n_col - 1)
            return found + (home == mine).astype(jnp.int32)

        asked = repeat(queries, ask)
        clear(has_ref, 0)
        x_ref[...] = jnp.zeros(x_ref.shape, BF16)
        place_of = lax.broadcasted_iota(jnp.int32, (PLACES, tile), 0)
        node_of = lax.broadcasted_iota(jnp.int32, (PLACES, tile), 1)

        def mark_query(place, carry):
            node = asked_ref[first + place]
            block = (node >> (tile_bits + block_bits + col_bits)) * BPD + ((node >> tile_bits) & (BPD - 1))
            here = (place_of == place) & (node_of == (node & (tile - 1)))
            x_ref[block] = jnp.where(here, 1.0, x_ref[block].astype(F32)).astype(BF16)
            has_ref[block] = 1
            return carry

        lax.fori_loop(0, jnp.clip(asked - first, 0, PLACES), mark_query, 0)

        def pick(index, found):
            list_ref[found] = index
            return found + jnp.where(index < live, has_ref[col_ref[index]], 0)

        found = repeat(slots, pick)

        def start(lane, carry):
            copy(list_ref[lane], lane).start()
            return carry

        lax.fori_loop(0, found, start, 0)
        clear(mark_ref, 0)

        def mark_row(index, carry):
            mark_ref[jnp.where(index < live, row_ref[index], row_blocks)] = 1
            return carry

        repeat(slots, mark_row)
        clear(id_ref, BPD)
        id_rows_ref[...] = jnp.full(id_rows_ref.shape, float(BPD), F32)

        def number_owner(owner, sent_to):
            rank = 0
            for block in range(BPD):
                marked = mark_ref[owner * BPD + block]
                slot_ref[owner * BPD + block] = sent_to * TOUCH + rank
                id_ref[sent_to * TOUCH + rank] = jnp.where(marked > 0, block, BPD)
                rank = rank + marked
            for place in range(TOUCH):
                number = id_ref[sent_to * TOUCH + place].astype(F32)
                id_rows_ref[sent_to, place : place + 1] = jnp.full((1, tile), number, F32)

        for sent_to, owner in enumerate(exchange_order(n_col)):
            number_owner(owner, sent_to)
        acc_ref[...] = jnp.zeros(acc_ref.shape, F32)

        def step(index, carry):
            prods, goes = [], []
            for lane in range(FIRST_UNROLL):
                at = index * FIRST_UNROLL + lane
                valid = at < found
                which = jnp.where(valid, list_ref[at], 0)

                @pl.when(valid)
                def _():
                    copy(which, at).wait()

                goes.append((at, which, valid))
            for at, which, valid in goes:
                prods.append(
                    lax.dot_general(
                        x_ref[col_ref[which]], tile_ref[at], (((1,), (1,)), ((), ())), preferred_element_type=F32
                    )
                )
            for (at, which, valid), prod in zip(goes, prods):
                slot = jnp.where(valid, slot_ref[row_ref[which]], spare)
                acc_ref[slot] = acc_ref[slot] + prod
            return carry

        lax.fori_loop(0, (found + FIRST_UNROLL - 1) // FIRST_UNROLL, step, 0)
        out_ref[:, :sent_rows] = acc_ref[:spare].reshape(n_col, sent_rows, tile).astype(BF16)
        out_ref[:, sent_rows:] = id_rows_ref[...].astype(BF16)

    info = jnp.stack([count, col, round_index]).astype(jnp.int32)
    return pl.pallas_call(
        body,
        out_shape=jax.ShapeDtypeStruct((n_col, sent_rows + ID_ROWS, tile), BF16),
        in_specs=[SMEM, SMEM, SMEM, SMEM, HBM],
        out_specs=VMEM,
        scratch_shapes=[
            pltpu.VMEM((spare + 1, PLACES, tile), F32),
            pltpu.VMEM((col_blocks, PLACES, tile), BF16),
            pltpu.VMEM(tiles.shape, tiles.dtype),
            pltpu.VMEM((n_col, ID_ROWS, tile), F32),
            pltpu.SMEM((queries,), jnp.int32),
            pltpu.SMEM((col_blocks,), jnp.int32),
            pltpu.SMEM((slots,), jnp.int32),
            pltpu.SMEM((row_blocks + 8,), jnp.int32),
            pltpu.SMEM((row_blocks,), jnp.int32),
            pltpu.SMEM((spare + 8,), jnp.int32),
            pltpu.SemaphoreType.DMA((slots,)),
        ],
        compiler_params=PARAMS,
        name="first_products",
    )(info, rows, cols, query_ids, pltpu.with_memory_space_constraint(tiles, pltpu.HBM))


def products(step, slots, places, count, turned, xparts, owners, damping, owned, scores):
    parts = len(xparts)
    each, width, tile = xparts[0].shape
    rows = TOUCH * width
    before = [] if step == 1 else [scores]

    def body(slot_ref, place_ref, count_ref, tiles_ref, *refs):
        x_refs, (damping_ref, owned_ref), refs = refs[:parts], refs[parts : parts + 2], refs[parts + 2 :]
        score_in, refs = refs[: len(before)], refs[len(before) :]
        out_ref, score_out, score_ref, score_sems, acc_ref, *scratch = refs
        for ref in score_in:
            pltpu.make_async_copy(ref, score_ref, score_sems.at[0]).start()
        leave = pltpu.make_async_copy(score_ref, score_out, score_sems.at[1])

        def add_scores():
            for ref in score_in:
                pltpu.make_async_copy(ref, score_ref, score_sems.at[0]).wait()
            if score_in:
                score_ref[...] = score_ref[...] + power(damping_ref, step - 1)[None] * owned_ref[...]
            else:
                score_ref[...] = owned_ref[...]
            leave.start()

        multiply_tiles(slot_ref, place_ref, count_ref[0], tiles_ref, x_refs, acc_ref, *scratch, add_scores)
        out_ref[...] = acc_ref[: owners * TOUCH].astype(BF16).reshape(owners, rows, tile)
        leave.wait()

    return pl.pallas_call(
        body,
        out_shape=(
            jax.ShapeDtypeStruct((owners, rows, tile), BF16),
            pltpu.HBM((BPD, width, tile), F32),
        ),
        in_specs=[SMEM, SMEM, SMEM, VMEM] + [VMEM] * (parts + 2) + [HBM] * len(before),
        out_specs=(VMEM, HBM),
        scratch_shapes=[
            pltpu.VMEM((BPD, width, tile), F32),
            pltpu.SemaphoreType.DMA((2,)),
            pltpu.VMEM((owners * TOUCH + 1, width, tile), F32),
            pltpu.VMEM((parts * each, width, tile), BF16),
        ],
        compiler_params=PARAMS,
        name="products",
    )(
        slots,
        places,
        count,
        turned,
        *xparts,
        damping,
        owned,
        *[pltpu.with_memory_space_constraint(part, pltpu.HBM) for part in before],
    )


def turned_tiles(count, tiles):
    def body(count_ref, tiles_ref, out_ref):
        def group(index, carry):
            for lane in range(UNROLL):
                out_ref[index * UNROLL + lane] = jnp.transpose(tiles_ref[index * UNROLL + lane])
            return carry

        lax.fori_loop(0, (count_ref[0] + UNROLL - 1) // UNROLL, group, 0)

    return pl.pallas_call(
        body,
        out_shape=jax.ShapeDtypeStruct(tiles.shape, tiles.dtype),
        in_specs=[SMEM, VMEM],
        out_specs=VMEM,
        compiler_params=PARAMS,
        name="turned",
    )(count, tiles)


def summed(id_ref, got_ref, acc_ref):
    width = acc_ref.shape[1]
    acc_ref[...] = jnp.zeros(acc_ref.shape, F32)
    for source in range(got_ref.shape[0]):
        for place in range(TOUCH):
            block = id_ref[source * TOUCH + place]
            part = got_ref[source, place * width : (place + 1) * width].astype(F32)
            acc_ref[block] = acc_ref[block] + part


def owned_sum(ids, got, damping):
    width, tile = damping.shape

    def body(id_ref, got_ref, x_ref, out_ref, acc_ref):
        summed(id_ref, got_ref, acc_ref)
        owned = acc_ref[:BPD]
        x_ref[...] = owned.astype(BF16)
        out_ref[...] = owned

    return pl.pallas_call(
        body,
        out_shape=(
            jax.ShapeDtypeStruct((BPD, width, tile), BF16),
            jax.ShapeDtypeStruct((BPD, width, tile), F32),
        ),
        in_specs=[SMEM, VMEM],
        out_specs=(VMEM, VMEM),
        scratch_shapes=[pltpu.VMEM((BPD + 1, width, tile), F32)],
        compiler_params=PARAMS,
        cost_estimate=COVER,
        name="owned",
    )(ids, got)


def placed_sum(ids, got, spread, width, before=()):
    sources, _, tile = got.shape
    queries, columns = spread.shape
    streams = queries // width

    def body(id_ref, got_ref, spread_ref, *refs):
        whole_refs, out_refs, piece_ref = refs[: len(before)], refs[len(before) : -1], refs[-1]
        piece_ref[...] = jnp.zeros(piece_ref.shape, F32)
        for source in range(sources):
            part = got_ref[source].astype(F32)
            for place in range(TOUCH):
                block = id_ref[source * TOUCH + place]
                piece_ref[block, source * PLACES : (source + 1) * PLACES] = part[
                    place * PLACES : (place + 1) * PLACES
                ]
        for block in range(BPD):
            owned = jnp.dot(spread_ref[...], piece_ref[block].astype(BF16), preferred_element_type=F32)
            for stream in range(streams):
                mine = owned[stream * width : (stream + 1) * width]
                if whole_refs:
                    mine = mine + whole_refs[stream][block]
                out_refs[stream][block] = mine

    shape = (BPD, width, tile)
    return pl.pallas_call(
        body,
        out_shape=[jax.ShapeDtypeStruct(shape, F32)] * streams,
        in_specs=[SMEM] + [VMEM] * (2 + len(before)),
        out_specs=[VMEM] * streams,
        scratch_shapes=[pltpu.VMEM((BPD + 1, columns, tile), F32)],
        compiler_params=PARAMS,
        name="placed",
    )(ids, got, spread, *before)


def rounded(whole):
    def body(whole_ref, out_ref):
        out_ref[...] = whole_ref[...].astype(BF16)

    return pl.pallas_call(
        body,
        out_shape=jax.ShapeDtypeStruct(whole.shape, BF16),
        in_specs=[VMEM],
        out_specs=VMEM,
        compiler_params=PARAMS,
        cost_estimate=COVER,
        name="rounded",
    )(whole)


def ended_sum(step, ids, got, damping, scores):
    width, tile = damping.shape

    def body(id_ref, got_ref, damping_ref, score_ref, out_ref, acc_ref):
        summed(id_ref, got_ref, acc_ref)
        out_ref[...] = score_ref[...] + power(damping_ref, step)[None] * acc_ref[:BPD]

    return pl.pallas_call(
        body,
        out_shape=jax.ShapeDtypeStruct((BPD, width, tile), F32),
        in_specs=[SMEM] + [VMEM] * 3,
        out_specs=VMEM,
        scratch_shapes=[pltpu.VMEM((BPD + 1, width, tile), F32)],
        compiler_params=PARAMS,
        name="ended",
    )(ids, got, damping, scores)


def last_sum(step, ids, got, damping, scores, *done):
    width, tile = damping.shape
    queries = sum(part.shape[1] for part in done) + width

    def body(id_ref, got_ref, damping_ref, score_ref, *refs):
        done_refs, (out_ref, acc_ref, block_ref, sems) = refs[:-4], refs[-4:]
        summed(id_ref, got_ref, acc_ref)
        coef = power(damping_ref, step)
        leaving = []
        for block in range(BPD):
            mine = score_ref[block] + coef * acc_ref[block]
            rows = [part[block] for part in done_refs] + [mine]
            block_ref[block] = jnp.transpose(jnp.concatenate(rows, axis=0))
            leaving.append(pltpu.make_async_copy(block_ref.at[block], out_ref.at[block], sems.at[block]))
            leaving[-1].start()
        for copy in leaving:
            copy.wait()

    return pl.pallas_call(
        body,
        out_shape=pltpu.HBM((BPD, tile, queries), F32),
        in_specs=[SMEM] + [VMEM] * (3 + len(done)),
        out_specs=HBM,
        scratch_shapes=[
            pltpu.VMEM((BPD + 1, width, tile), F32),
            pltpu.VMEM((BPD, tile, queries), F32),
            pltpu.SemaphoreType.DMA((BPD,)),
        ],
        compiler_params=PARAMS,
        name="last",
    )(ids, got, damping, scores, *done)


def row_shift(dz, dcore):
    return [
        (z * N_CORE + core, (z + dz) % N_Z * N_CORE + (core + dcore) % N_CORE)
        for z in range(N_Z)
        for core in range(N_CORE)
    ]


def column_parts(mine):
    same = [mine] + [lax.ppermute(mine, "row", row_shift(dz, 0)) for dz in range(1, N_Z)]
    other = [lax.ppermute(part, "row", row_shift(0, 1)) for part in same]
    return same + other


def after(value, *others):
    return lax.optimization_barrier((value, *others))[0]


def exchange_order(n_col):
    n_y = n_col // N_X
    return [x * n_y + (y if x % 2 == 0 else n_y - 1 - y) for x in range(N_X) for y in range(n_y)]


def position_of(device, n_col):
    n_y = n_col // N_X
    x, y = device // n_y, device % n_y
    return x * n_y + jnp.where(x % 2 == 0, y, n_y - 1 - y)


def exchange(sent):
    return lax.all_to_all(
        sent, "col", split_axis=0, concat_axis=0, tiled=True, axis_index_groups=[exchange_order(sent.shape[0])]
    )


def routes(rows, cols, count, n_col):
    slots = rows.shape[0]
    live = jnp.arange(slots, dtype=jnp.int32) < count
    blocks = jnp.arange(n_col * BPD, dtype=jnp.int32)
    hits = (rows[None, :] == blocks[:, None]) & live[None, :]
    marked = jnp.any(hits, axis=1).astype(jnp.int32).reshape(n_col, BPD)
    local = jnp.arange(BPD, dtype=jnp.int32)
    rank = jnp.sum(marked[:, None, :] * (local[None, None, :] < local[None, :, None]), axis=2)
    slot_of = (position_of(jnp.arange(n_col, dtype=jnp.int32), n_col)[:, None] * TOUCH + rank).reshape(-1)
    slot = jnp.sum(jnp.where(hits, slot_of[:, None], 0), axis=0)
    slot = jnp.where(live, slot, n_col * TOUCH)
    row = lax.axis_index("row")
    owner, block = cols // BPD, cols % BPD
    far = (row // N_CORE - owner // N_CORE) % N_Z
    place = ((row % N_CORE != owner % N_CORE).astype(jnp.int32) * N_Z + far) * BPD + block
    return slot, place


def shards(tiles, tile_row, tile_col, tile_count, query_ids, damping):
    tiles, rows, cols, count = tiles[0, 0], tile_row[0, 0], tile_col[0, 0], tile_count[0, 0]
    tile = tiles.shape[1]
    queries = query_ids.shape[0]
    width = queries // STREAMS
    n_row, n_col = lax.axis_size("row"), lax.axis_size("col")
    col = lax.axis_index("col")

    def first_sent(round_index):
        return first_products(round_index, rows, cols, query_ids, count, col, tiles, n_col, n_row)

    sent = first_sent(0)
    got = exchange(sent)

    later_ids = after(query_ids, sent)
    home = later_ids // (BPD * tile) % n_col
    number = jnp.arange(queries, dtype=jnp.int32)
    same_home = home[:, None] == home[None, :]
    rank = jnp.sum((same_home & (number[None, :] < number[:, None])).astype(jnp.int32), axis=1)
    rounds = jnp.max(rank) // PLACES + 1

    def spread(round_index):
        place = rank - round_index * PLACES
        column = jnp.where((place >= 0) & (place < PLACES), position_of(home, n_col) * PLACES + place, -1)
        return (column[:, None] == jnp.arange(n_col * PLACES, dtype=jnp.int32)[None, :]).astype(BF16)

    slot, place = routes(after(rows, sent), cols, count, n_col)
    turned = turned_tiles(count.reshape(1), after(tiles, sent))
    first_spread = spread(0)
    got_ids = got[:, -ID_ROWS:, 0][:, :TOUCH].astype(jnp.int32).reshape(-1)
    sums = placed_sum(got_ids, after(got, turned, slot, place, first_spread), first_spread, width)

    def next_round(state):
        index, *sums = state
        got = exchange(first_sent(index))
        return index + 1, *placed_sum(got_ids, got, spread(index), width, sums)

    _, *sums = lax.while_loop(lambda state: state[0] < rounds, next_round, (jnp.int32(1), *sums))
    count = count.reshape(1)
    dampings = [
        jnp.broadcast_to(damping[stream * width : (stream + 1) * width][:, None], (width, tile))
        for stream in range(STREAMS)
    ]
    xparts = [None] * STREAMS
    owned, scores = sums, [None] * STREAMS
    for step in range(1, TERMS):
        for stream in range(STREAMS):
            if step == 1:
                mine = rounded(after(owned[stream], sent) if stream else owned[stream])
                xparts[stream] = column_parts(mine)
            sent, scores[stream] = products(
                step,
                slot,
                place,
                count,
                turned,
                xparts[stream],
                n_col,
                dampings[stream],
                owned[stream],
                scores[stream],
            )
            got = exchange(sent)
            if step + 1 < TERMS:
                mine, owned[stream] = owned_sum(got_ids, got, dampings[stream])
                xparts[stream] = column_parts(mine)
            elif stream + 1 < STREAMS:
                scores[stream] = ended_sum(step, got_ids, got, dampings[stream], scores[stream])
            else:
                total = last_sum(step, got_ids, got, dampings[stream], scores[stream], *scores[:-1])
    return total.reshape(BPD * tile, -1)


def solution(mesh):
    in_specs = (
        P("row", "col", None, None, None),
        P("row", "col", None),
        P("row", "col", None),
        P("row", "col"),
        P(),
        P(),
    )
    out_specs = P(("row", "col"), None)
    return jax.shard_map(shards, mesh=mesh, in_specs=in_specs, out_specs=out_specs, check_vma=False)
```
